32 devices in a mesh: seq: 8 (over y, x, core), zero: 4 (over z).
Axes of the slice: x: 2, y: 2, z: 4, core: 2. Of those that a mesh axis runs over, the one named last changes fastest.
Arguments:
- hidden: bfloat16 [4, 1024, 1280], P('zero', 'seq'), may hold values from -6 to 6
- output_grad: bfloat16 [4, 1024, 2560], P('zero', 'seq'), may hold values from -6 to 6
- input_weight: bfloat16 [1280, 2856], P('zero'), may hold values from -0.15625 to 0.15625
- step_bias: float32 [40], replicated, may hold values from -7 to -2
- decay_log: float32 [40], replicated, may hold values from -4 to 1
- skip_gain: float32 [40], replicated, may hold values from 0.5 to 1.5
Outputs:
- hidden_grad: bfloat16 [4, 1024, 1280], P('zero', 'seq')
- weight_grad: float32 [1280, 2856], P(('seq', 'zero'))
- head_grads: float32 [3, 40], replicated
The draws below stay inside these ranges and needn't reach their ends.
All inputs are finite; a program needn't handle non-finite values.
Results may differ from the reference program's by a relative error of at most 0.0049.
Values may be sent and summed in bfloat16 or wider, within the bound.
A program may use at most 192 MiB of HBM per device.

```python
import jax
import jax.numpy as jnp
from jax import lax

D = 1280
HEADS = 40
HEAD_DIM = 64
STATE = 128
GROUP = 128
INNER = 2560
PROJ = 2856
LENGTH = 1024
SEQS = 4


def levels(key, shape, split, smallest, top_value):
    loudness = 1.0
    for position, blocks in split:
        steps = jax.random.uniform(jax.random.fold_in(jax.random.fold_in(key, 6), position), (blocks,), jnp.float32, smallest / len(split), top_value / len(split))
        loudness = loudness * jnp.repeat(jnp.exp(steps), shape[position] // blocks).reshape((-1,) + (1,) * (len(shape) - 1 - position))
    return loudness


def normal_values(stream_key, shape, deviation, bound, split=(), dtype=jnp.bfloat16):
    drawn = jax.random.normal(stream_key, shape, jnp.float32) * deviation
    if len(split) > 0:
        drawn = levels(stream_key, shape, split, -0.22, 0.18) * drawn
    return jnp.clip(drawn, min=-bound, max=bound).astype(dtype)


def setup_inputs(seed: int = 0) -> dict:
    seeds = jax.random.split(jax.random.key(seed), 7)
    return {
        "hidden": normal_values(seeds[0], (SEQS, LENGTH, D), 1.0, 6.0, ((0, 4), (1, 8))),
        "output_grad": normal_values(seeds[1], (SEQS, LENGTH, INNER), 1.0, 6.0, ((0, 4), (1, 8))),
        "input_weight": normal_values(seeds[2], (D, PROJ), D ** -0.5, 0.15625, ((0, 4),)),
        "step_bias": jnp.clip(jax.random.uniform(seeds[3], (HEADS,), jnp.float32, -7.0, -2.0), -7.0, -2.0),
        "decay_log": jnp.clip(jax.random.uniform(seeds[4], (HEADS,), jnp.float32, -4.0, 1.0), -4.0, 1.0),
        "skip_gain": jnp.clip(jax.random.uniform(seeds[5], (HEADS,), jnp.float32, 0.5, 1.5), 0.5, 1.5),
    }


highest = lax.Precision.HIGHEST

def state_mixer(columns, step_bias, decay_log, skip_gain, initial):
    length = columns.shape[0]
    blocks = length // GROUP
    values = jax.nn.silu(columns[:, :INNER])
    input_map = jax.nn.silu(columns[:, INNER:INNER + STATE]).reshape(blocks, GROUP, STATE)
    output_map = jax.nn.silu(columns[:, INNER + STATE:INNER + 2 * STATE]).reshape(blocks, GROUP, STATE)
    step_size = jax.nn.softplus(columns[:, INNER + 2 * STATE:] + step_bias)
    log_decay = -jnp.exp(decay_log) * step_size
    head_values = values.reshape(blocks, GROUP, HEADS, HEAD_DIM)
    scaled = head_values * step_size.reshape(blocks, GROUP, HEADS)[:, :, :, None]
    cumulative = jnp.cumsum(log_decay.reshape(blocks, GROUP, HEADS), axis=1)
    causal = (lax.broadcasted_iota(jnp.int32, (GROUP, GROUP), 0) >= lax.broadcasted_iota(jnp.int32, (GROUP, GROUP), 1))[None, :, :, None]
    differences = cumulative[:, :, None, :] - cumulative[:, None, :, :]
    within = jnp.where(causal, jnp.exp(jnp.where(causal, differences, 0.0)), 0.0)
    scores = jnp.einsum('kqn,ksn->kqs', output_map, input_map, precision=highest)
    inside = jnp.einsum('kqsh,kshp->kqhp', scores[:, :, :, None] * within, scaled, precision=highest)
    tail_decay = jnp.exp(cumulative[:, -1:, :] - cumulative)
    group_states = jnp.einsum('kshp,ksn->khpn', scaled * tail_decay[:, :, :, None], input_map, precision=highest)
    totals = cumulative[:, -1, :]

    def advance(running, inputs):
        block_total, block_state = inputs
        return (jnp.exp(block_total)[:, None, None] * running + block_state, running)
    final_state, entering = lax.scan(advance, initial, (totals, group_states))
    from_state = jnp.einsum('kqn,khpn->kqhp', output_map, entering, precision=highest) * jnp.exp(cumulative)[:, :, :, None]
    mixed_out = inside + from_state + skip_gain[None, None, :, None] * head_values
    return (mixed_out.reshape(length, INNER), final_state, lax.optimization_barrier(jnp.sum(totals, axis=0)))

def reference(hidden, output_grad, input_weight, step_bias, decay_log, skip_gain):
    initial = jnp.zeros((HEADS, HEAD_DIM, STATE), jnp.float32)

    def one_sequence(running, inputs):
        weight_sum, head_sum = running
        tokens, cotangent = inputs
        projected = jnp.dot(tokens, input_weight, preferred_element_type=jnp.float32)

        def forward(columns, bias_part, log_part, gain_part):
            return state_mixer(columns, bias_part, log_part, gain_part, initial)[0]
        unused, pullback = jax.vjp(forward, projected, step_bias, decay_log, skip_gain)
        column_grad, bias_grad, log_grad, gain_grad = pullback(cotangent.astype(jnp.float32))
        rounded = column_grad.astype(jnp.bfloat16)
        token_grad = lax.dot_general(rounded, input_weight, (((1,), (1,)), ((), ())), preferred_element_type=jnp.float32).astype(jnp.bfloat16)
        weight_sum = weight_sum + lax.dot_general(tokens, rounded, (((0,), (0,)), ((), ())), preferred_element_type=jnp.float32)
        head_sum = head_sum + jnp.stack([bias_grad, log_grad, gain_grad])
        return ((weight_sum, head_sum), token_grad)
    starting = (jnp.zeros((D, PROJ), jnp.float32), jnp.zeros((3, HEADS), jnp.float32))
    (weight_grad, head_grads), hidden_grad = lax.scan(one_sequence, starting, (hidden, output_grad))
    return (hidden_grad, weight_grad, head_grads)
```

```python
import functools

import jax
import jax.numpy as jnp
from jax import lax
from jax.experimental import pallas as pl
from jax.experimental.pallas import tpu as pltpu
from jax.sharding import PartitionSpec as P

HEAD_DIM = 64
STATE = 128
MESH = pl.DeviceIdType.MESH
F32 = jnp.float32
BF16 = jnp.bfloat16


def up(size, unit):
    return -(-size // unit) * unit


def nn(a, b):
    return lax.dot_general(a, b, (((1,), (0,)), ((), ())), preferred_element_type=F32)


def nt(a, b):
    return lax.dot_general(a, b, (((1,), (1,)), ((), ())), preferred_element_type=F32)


def tn(a, b):
    return lax.dot_general(a, b, (((0,), (0,)), ((), ())), preferred_element_type=F32)


def exact(a, b):
    return lax.dot_general(
        a, b, (((1,), (0,)), ((), ())), precision=lax.Precision.HIGHEST, preferred_element_type=F32
    )


def greet(peers):
    barrier = pltpu.get_barrier_semaphore()
    total = 0
    for count, peer in peers:

        def one(step, carry, peer=peer):
            pl.semaphore_signal(barrier, inc=1, device_id=peer(step), device_id_type=MESH)
            return carry

        lax.fori_loop(1, count, one, 0)
        total += count - 1
    pl.semaphore_wait(barrier, total)


def run_copies(copies, locals_):
    for copy in locals_:
        copy.start()
    for count, make in copies:
        lax.fori_loop(1, count, lambda step, c, make=make: (make(step).start(), c)[1], 0)
    for copy in locals_:
        copy.wait()
    for count, make in copies:
        lax.fori_loop(1, count, lambda step, c, make=make: (make(step).wait(), c)[1], 0)


def collect_kernel(seqs, zeros, tok, cot, wgt, tok_out, cot_out, wgt_out, send, recv, wsend, wrecv, loc):
    me_s, me_z = lax.axis_index("seq"), lax.axis_index("zero")

    def along_seq(step):
        return (lax.rem(me_s + step, seqs), me_z)

    def along_zero(step):
        return (me_s, lax.rem(me_z + step, zeros))

    def token_copy(step):
        return pltpu.make_async_remote_copy(
            tok, tok_out.at[me_s], send.at[0, step], recv.at[0, step], along_seq(step), MESH
        )

    def cot_copy(step):
        target = along_seq(step)
        return pltpu.make_async_remote_copy(
            cot.at[target[0]], cot_out.at[me_s], send.at[1, step], recv.at[1, step], target, MESH
        )

    def weight_copy(step):
        return pltpu.make_async_remote_copy(
            wgt, wgt_out.at[me_z], wsend.at[step], wrecv.at[step], along_zero(step), MESH
        )

    greet(((seqs, along_seq), (zeros, along_zero)))
    run_copies(
        ((zeros, weight_copy), (seqs, token_copy), (seqs, cot_copy)),
        (
            pltpu.make_async_copy(tok, tok_out.at[me_s], loc.at[0]),
            pltpu.make_async_copy(cot.at[me_s], cot_out.at[me_s], loc.at[1]),
            pltpu.make_async_copy(wgt, wgt_out.at[me_z], loc.at[2]),
        ),
    )


def collect(tok, cot, wgt, seqs, zeros):
    anywhere = pl.BlockSpec(memory_space=pl.ANY)
    return pl.pallas_call(
        functools.partial(collect_kernel, seqs, zeros),
        out_shape=(
            jax.ShapeDtypeStruct((seqs,) + tok.shape, tok.dtype),
            jax.ShapeDtypeStruct(cot.shape, cot.dtype),
            jax.ShapeDtypeStruct((zeros,) + wgt.shape, wgt.dtype),
        ),
        in_specs=[anywhere] * 3,
        out_specs=(anywhere,) * 3,
        scratch_shapes=[
            pltpu.SemaphoreType.DMA((2, seqs)),
            pltpu.SemaphoreType.DMA((2, seqs)),
            pltpu.SemaphoreType.DMA((zeros,)),
            pltpu.SemaphoreType.DMA((zeros,)),
            pltpu.SemaphoreType.DMA((3,)),
        ],
        compiler_params=pltpu.CompilerParams(collective_id=0, has_side_effects=True),
        name="collect",
    )(tok, cot, wgt)


def deliver_kernel(seqs, zeros, tok, wgt, head, tok_out, wgt_out, head_out, tsend, trecv, send, recv, loc):
    me_s, me_z = lax.axis_index("seq"), lax.axis_index("zero")
    every = seqs * zeros
    me = me_s * zeros + me_z

    def along_seq(step):
        return (lax.rem(me_s + step, seqs), me_z)

    def anyone(step):
        target = lax.rem(me + step, every)
        return (target // zeros, lax.rem(target, zeros))

    def token_copy(step):
        target = along_seq(step)
        return pltpu.make_async_remote_copy(
            tok.at[target[0]], tok_out.at[me_s], tsend.at[step], trecv.at[step], target, MESH
        )

    def weight_copy(step):
        target = lax.rem(me + step, every)
        return pltpu.make_async_remote_copy(
            wgt.at[target], wgt_out.at[me], send.at[0, step], recv.at[0, step], anyone(step), MESH
        )

    def head_copy(step):
        return pltpu.make_async_remote_copy(
            head, head_out.at[me], send.at[1, step], recv.at[1, step], anyone(step), MESH
        )

    greet(((every, anyone),))
    run_copies(
        ((seqs, token_copy), (every, weight_copy), (every, head_copy)),
        (
            pltpu.make_async_copy(tok.at[me_s], tok_out.at[me_s], loc.at[0]),
            pltpu.make_async_copy(wgt.at[me], wgt_out.at[me], loc.at[1]),
            pltpu.make_async_copy(head, head_out.at[me], loc.at[2]),
        ),
    )


def deliver(tok, wgt, head, seqs, zeros):
    anywhere = pl.BlockSpec(memory_space=pl.ANY)
    every = seqs * zeros
    return pl.pallas_call(
        functools.partial(deliver_kernel, seqs, zeros),
        out_shape=(
            jax.ShapeDtypeStruct(tok.shape, tok.dtype),
            jax.ShapeDtypeStruct(wgt.shape, wgt.dtype),
            jax.ShapeDtypeStruct((every,) + head.shape, head.dtype),
        ),
        in_specs=[anywhere] * 3,
        out_specs=(anywhere,) * 3,
        scratch_shapes=[
            pltpu.SemaphoreType.DMA((seqs,)),
            pltpu.SemaphoreType.DMA((seqs,)),
            pltpu.SemaphoreType.DMA((2, every)),
            pltpu.SemaphoreType.DMA((2, every)),
            pltpu.SemaphoreType.DMA((3,)),
        ],
        compiler_params=pltpu.CompilerParams(collective_id=1, has_side_effects=True),
        name="deliver",
    )(tok, wgt, head)


def mixer_kernel(hp, pre_ref, dy_ref, par_ref, g_ref, head_ref, states, grad, acc):
    chunks, inner, group = dy_ref.shape
    top = inner + 2 * STATE
    slots = acc.shape[1]
    bias = par_ref[0][:, :1]
    rate = -jnp.exp(par_ref[1][:, :1])
    gain = par_ref[2][:, :1]
    row = lax.broadcasted_iota(jnp.int32, (group, group), 0)
    col = lax.broadcasted_iota(jnp.int32, (group, group), 1)
    causal = col >= row
    before = causal.astype(F32)
    after = (col <= row).astype(F32)

    def spread(rows):
        return jnp.concatenate(
            [jnp.broadcast_to(rows[h : h + 1], (HEAD_DIM, rows.shape[1])) for h in range(hp)], axis=0
        )

    def gather_rows(full):
        parts = [
            jnp.sum(full[h * HEAD_DIM : (h + 1) * HEAD_DIM], axis=0, keepdims=True) for h in range(hp)
        ]
        if slots > hp:
            parts.append(jnp.zeros((slots - hp, full.shape[1]), F32))
        return jnp.concatenate(parts, axis=0)

    def load(k):
        at = pl.ds(pl.multiple_of(k * group, group), group)
        pre = pre_ref[:inner, at]
        sig = jax.nn.sigmoid(pre)
        maps = pre_ref[inner:top, at]
        map_sig = jax.nn.sigmoid(maps)
        raw = pre_ref[top : top + slots, at] + bias
        step = jax.nn.softplus(raw)
        cum = exact(rate * step, before)
        return at, pre, sig, maps, map_sig, raw, step, cum

    grad[...] = jnp.zeros_like(grad)

    def forward(k, carry):
        at, pre, sig, maps, map_sig, raw, step, cum = load(k)
        last = cum[:, group - 1 :]
        x = pre * sig
        in_map = (maps[:STATE] * map_sig[:STATE]).astype(BF16)
        tail = (x * spread(step * jnp.exp(last - cum))).astype(BF16)
        held = grad[...]
        states[k] = held
        grad[...] = spread(jnp.exp(jnp.broadcast_to(last, (slots, STATE)))) * held + nt(tail, in_map)
        return carry

    lax.fori_loop(0, chunks, forward, 0)
    grad[...] = jnp.zeros_like(grad)
    acc[...] = jnp.zeros_like(acc)

    def backward(i, carry):
        k = chunks - 1 - i
        at, pre, sig, maps, map_sig, raw, step, cum = load(k)
        last = cum[:, group - 1 :]
        x = pre * sig
        both = maps * map_sig
        in_map = both[:STATE].astype(BF16)
        out_map = both[STATE:].astype(BF16)
        dy16 = dy_ref[k]
        dy = dy16.astype(F32)
        u = x * spread(step)
        u16 = u.astype(BF16)
        tail = spread(jnp.exp(last - cum))
        lead = spread(jnp.exp(cum))
        leave = spread(jnp.exp(jnp.broadcast_to(last, (slots, STATE))))
        held = states[k]
        held16 = held.astype(BF16)
        g_out = grad[...]
        g16 = g_out.astype(BF16)
        u_tail16 = (u * tail).astype(BF16)
        dy_lead = dy * lead
        dy_lead16 = dy_lead.astype(BF16)

        score = tn(in_map, out_map)
        cum_col = jnp.concatenate([cum, jnp.zeros((group - slots, group), F32)], axis=0).T
        d_score = jnp.zeros((group, group), F32)
        ksum = jnp.zeros((group, group), F32)
        du_parts = []
        r_parts = []
        for h in range(hp):
            at_h = slice(h * HEAD_DIM, (h + 1) * HEAD_DIM)
            diff = cum[h : h + 1] - cum_col[:, h : h + 1]
            within = jnp.where(causal, jnp.exp(jnp.where(causal, diff, 0.0)), 0.0)
            mixing = score * within
            d_mix = tn(u16[at_h], dy16[at_h])
            du_parts.append(nt(dy16[at_h], mixing.astype(BF16)))
            d_score = d_score + d_mix * within
            pair = d_mix * mixing
            r_parts.append(jnp.sum(pair, axis=0, keepdims=True))
            ksum = jnp.where(col == h, jnp.sum(pair, axis=1, keepdims=True), ksum)
        if slots > hp:
            r_parts.append(jnp.zeros((slots - hp, group), F32))
        from_tail = nn(g16, in_map) * tail
        tail_rows = gather_rows(u * from_tail)
        lead_rows = gather_rows(dy_lead * nn(held16, out_map))
        du = jnp.concatenate(du_parts, axis=0) + from_tail
        d_cum = jnp.concatenate(r_parts, axis=0) - ksum.T[:slots] + lead_rows - tail_rows
        cross = jnp.sum(gather_rows(held * g_out * leave) + tail_rows, axis=1, keepdims=True)
        d_log = exact(d_cum, after) + cross
        d_step = gather_rows(du * x) + rate * d_log
        d_raw = d_step * jax.nn.sigmoid(raw)

        d_score16 = d_score.astype(BF16)
        d_out = nn(in_map, d_score16) + tn(held16, dy_lead16)
        d_in = nt(out_map, d_score16) + tn(g16, u_tail16)
        grad[...] = leave * g_out + nt(dy_lead16, out_map)

        slope = sig * (1.0 + pre * (1.0 - sig))
        map_slope = map_sig * (1.0 + maps * (1.0 - map_sig))
        g_ref[:inner, at] = ((du * spread(step) + dy * gain_full) * slope).astype(BF16)
        g_ref[inner:top, at] = (jnp.concatenate([d_in, d_out], axis=0) * map_slope).astype(BF16)
        rest = g_ref.shape[0] - top
        g_ref[top:, at] = jnp.concatenate(
            [d_raw, jnp.zeros((rest - slots, group), F32)], axis=0
        ).astype(BF16)
        acc[0] += d_raw
        acc[1] += d_log * (rate * step)
        acc[2] += gather_rows(dy * x)
        return carry

    gain_full = spread(jnp.broadcast_to(gain, (slots, group)))
    lax.fori_loop(0, chunks, backward, 0)
    for i in range(3):
        head_ref[i] = jnp.broadcast_to(jnp.sum(acc[i], axis=1, keepdims=True), head_ref.shape[1:])


def mixer(pre, dy, par, hp):
    chunks, inner, group = dy.shape
    slots = par.shape[1]
    return pl.pallas_call(
        functools.partial(mixer_kernel, hp),
        out_shape=(
            jax.ShapeDtypeStruct(pre.shape, BF16),
            jax.ShapeDtypeStruct((3, slots, 128), F32),
        ),
        in_specs=[pl.BlockSpec(memory_space=pltpu.VMEM)] * 3,
        out_specs=(pl.BlockSpec(memory_space=pltpu.VMEM),) * 2,
        scratch_shapes=[
            pltpu.VMEM((chunks, inner, STATE), F32),
            pltpu.VMEM((inner, STATE), F32),
            pltpu.VMEM((3, slots, group), F32),
        ],
        compiler_params=pltpu.CompilerParams(vmem_limit_bytes=48 * 1024 * 1024),
        name="mixer",
    )(pre, dy, par)


def body(seqs, zeros, hidden, output_grad, input_weight, step_bias, decay_log, skip_gain):
    heads = step_bias.shape[0]
    hp = up(heads, seqs) // seqs
    slots = up(hp, 8)
    inner, full = hp * HEAD_DIM, heads * HEAD_DIM
    spare = seqs * hp - heads
    width = up(inner + 2 * STATE + slots, 128)
    me = lax.axis_index("seq")
    length, model = hidden.shape[1:]

    def own(array, axis, size, extra):
        if extra:
            pads = [(0, 0)] * array.ndim
            pads[axis] = (0, extra)
            array = jnp.pad(array, pads)
        return lax.dynamic_slice_in_dim(array, me * size, size, axis)

    weight = jnp.concatenate(
        [
            own(input_weight[:, :full], 1, inner, spare * HEAD_DIM),
            input_weight[:, full : full + 2 * STATE],
            own(input_weight[:, full + 2 * STATE :], 1, hp, spare),
            jnp.zeros((input_weight.shape[0], width - inner - 2 * STATE - hp), BF16),
        ],
        axis=1,
    )
    cot = jnp.pad(output_grad[0], ((0, 0), (0, spare * HEAD_DIM))).T.reshape(seqs, inner, length)
    par = jnp.stack([own(v, 0, hp, spare) for v in (step_bias, decay_log, skip_gain)])
    par = jnp.broadcast_to(jnp.pad(par, ((0, 0), (0, slots - hp)))[:, :, None], (3, slots, 128))

    tokens, dy, columns = collect(hidden[0], cot, weight, seqs, zeros)
    tokens = tokens.reshape(seqs * length, model)
    columns = columns.reshape(model, width)
    pre = lax.dot_general(columns, tokens, (((0,), (1,)), ((), ())), preferred_element_type=F32)
    grads, sums = mixer(pre, dy, par, hp)
    token_part = tn(grads, columns_t(columns)).astype(BF16).reshape(seqs, length, model)
    weight_part = lax.dot_general(
        tokens, grads, (((0,), (1,)), ((), ())), preferred_element_type=F32
    ).astype(BF16)
    every = seqs * zeros
    weight_part = weight_part.reshape(every, model // every, width)

    token_all, weight_all, sums_all = deliver(token_part, weight_part, sums, seqs, zeros)
    token_grad = jnp.sum(token_all.astype(F32), axis=0).astype(BF16)
    rows = jnp.sum(
        weight_all.reshape(seqs, zeros, model // every, width).astype(F32), axis=1
    )
    parts = rows.transpose(1, 0, 2)
    weight_grad = jnp.concatenate(
        [
            parts[:, :, :inner].reshape(-1, seqs * inner)[:, :full],
            jnp.sum(rows[:, :, inner : inner + 2 * STATE], axis=0),
            parts[:, :, inner + 2 * STATE : inner + 2 * STATE + hp].reshape(-1, seqs * hp)[:, :heads],
        ],
        axis=1,
    )
    sums_all = jnp.sum(sums_all.reshape(seqs, zeros, 3, slots, 128)[:, :, :, :hp, 0], axis=1)
    head_grads = sums_all.transpose(1, 0, 2).reshape(3, seqs * hp)[:, :heads]
    return (token_grad[None], weight_grad, head_grads)


def columns_t(columns):
    return columns.T


def solution(mesh):
    placed = (P("zero", "seq", None), P("zero", "seq", None), P("zero", None), P(), P(), P())
    return jax.shard_map(
        functools.partial(body, mesh.shape["seq"], mesh.shape["zero"]),
        mesh=mesh,
        in_specs=placed,
        out_specs=(P("zero", "seq", None), P(("seq", "zero"), None), P()),
        check_vma=False,
    )
```

```python
import functools

import jax
import jax.numpy as jnp
from jax import lax
from jax.experimental import pallas as pl
from jax.experimental.pallas import tpu as pltpu
from jax.sharding import PartitionSpec as P

HEAD_DIM = 64
STATE = 128
MESH = pl.DeviceIdType.MESH
F32 = jnp.float32
BF16 = jnp.bfloat16


def up(size, unit):
    return -(-size // unit) * unit


def nn(a, b):
    return lax.dot_general(a, b, (((1,), (0,)), ((), ())), preferred_element_type=F32)


def nt(a, b):
    return lax.dot_general(a, b, (((1,), (1,)), ((), ())), preferred_element_type=F32)


def tn(a, b):
    return lax.dot_general(a, b, (((0,), (0,)), ((), ())), preferred_element_type=F32)


def halves(a):
    high = a.astype(BF16)
    return high, (a - high.astype(F32)).astype(BF16)


def fine(dot, a, b):
    if a.dtype == BF16:
        high, low = halves(b)
        return dot(a, high) + dot(a, low)
    if b.dtype == BF16:
        high, low = halves(a)
        return dot(high, b) + dot(low, b)
    (ah, al), (bh, bl) = halves(a), halves(b)
    return dot(ah, bh) + (dot(al, bh) + dot(ah, bl))


def exact(a, b):
    return lax.dot_general(
        a, b, (((1,), (0,)), ((), ())), precision=lax.Precision.HIGHEST, preferred_element_type=F32
    )


def greet(peers):
    barrier = pltpu.get_barrier_semaphore()
    for peer in peers:
        pl.semaphore_signal(barrier, inc=1, device_id=peer, device_id_type=MESH)
    pl.semaphore_wait(barrier, len(peers))


def remote(src, dst, send, recv, peer):
    return pltpu.make_async_remote_copy(src, dst, send, recv, peer, MESH)


def collect_kernel(
    seqs, zeros, tok, cot, wgt, tok_out, cot_out, wgt_out, wsib_out,
    tsem, fsem, csem, rsem, ssem, loc,
):
    me_s, me_z = lax.axis_index("seq"), lax.axis_index("zero")
    chips = seqs // 2
    chip, core = me_s // 2, lax.rem(me_s, 2)
    sibling = (chip * 2 + 1 - core, me_z)
    half = wgt.shape[0] // 2
    full_hops = (zeros - 1) // 2
    upper, lower = pl.ds(0, half), pl.ds(half, wgt.shape[0] - half)

    def along(step):
        return (lax.rem(me_s + step, seqs), me_z)

    def owner(shift):
        return lax.rem(me_z + shift + zeros, zeros)

    right, left = (me_s, owner(1)), (me_s, owner(-1))
    greet([along(i) for i in range(1, seqs)] + ([right, left] if zeros > 1 else []))

    own = [
        pltpu.make_async_copy(tok, tok_out.at[me_s], loc.at[0]),
        pltpu.make_async_copy(cot.at[me_s], cot_out.at[me_s], loc.at[1]),
        pltpu.make_async_copy(wgt, wgt_out.at[me_z], loc.at[2]),
    ]

    def hop(way, h):
        at = owner(-way * (h - 1))
        src = wgt if h == 1 else wgt_out.at[at]
        dst = wgt_out.at[at]
        if h > full_hops:
            rows = upper if way > 0 else lower
            src, dst = src.at[rows], dst.at[rows]
        row = 0 if way > 0 else 2
        return remote(src, dst, rsem.at[row, h], rsem.at[row + 1, h], right if way > 0 else left)

    hops = full_hops + (1 - zeros % 2)
    ring = [(hop(1, h), hop(-1, h)) for h in range(1, hops + 1)]

    def token_slot(step):
        return lax.rem(chip - step + chips, chips) * 2 + core

    tokens = [
        remote(
            tok, tok_out.at[me_s], tsem.at[0, d], tsem.at[1, d],
            (lax.rem(chip + d, chips) * 2 + core, me_z),
        )
        for d in range(1, chips)
    ]
    cots = []
    for d in range(1, seqs):
        peer = along(d)
        cots.append(
            remote(cot.at[peer[0]], cot_out.at[me_s], csem.at[0, d], csem.at[1, d], peer)
        )
    passed = [remote(tok, tok_out.at[me_s], fsem.at[0, 0], fsem.at[1, 0], sibling)]
    for d in range(1, chips):
        at = token_slot(d)
        passed.append(remote(tok_out.at[at], tok_out.at[at], fsem.at[0, d], fsem.at[1, d], sibling))

    def share(slot, at, src):
        return remote(src, wsib_out.at[at], ssem.at[0, slot], ssem.at[1, slot], sibling)

    shared = [share(0, me_z, wgt)]
    for d in range(1, zeros):
        at = owner(-d)
        shared.append(share(d, at, wgt_out.at[at]))

    for copy in ring[0] if ring else ():
        copy.start()
    for copy in tokens + cots + [passed[0], shared[0]] + own:
        copy.start()
    for h in range(1, hops):
        for way in (0, 1):
            ring[h - 1][way].wait_recv()
            ring[h][way].start()
    for d in range(1, chips):
        tokens[d - 1].wait_recv()
        passed[d].start()
    if ring:
        for way in (0, 1):
            ring[-1][way].wait_recv()
    for copy in shared[1:]:
        copy.start()
    for pair in ring:
        for copy in pair:
            copy.wait_send()
    for copy in tokens:
        copy.wait_send()
    for copy in own + cots + passed + shared:
        copy.wait()


def collect(tok, cot, wgt, seqs, zeros):
    anywhere = pl.BlockSpec(memory_space=pl.ANY)
    columns = jax.ShapeDtypeStruct((zeros,) + wgt.shape, wgt.dtype)
    return pl.pallas_call(
        functools.partial(collect_kernel, seqs, zeros),
        out_shape=(
            jax.ShapeDtypeStruct((seqs,) + tok.shape, tok.dtype),
            jax.ShapeDtypeStruct(cot.shape, cot.dtype),
            columns,
            columns,
        ),
        in_specs=[anywhere] * 3,
        out_specs=(anywhere,) * 4,
        scratch_shapes=[
            pltpu.SemaphoreType.DMA((2, seqs)),
            pltpu.SemaphoreType.DMA((2, seqs)),
            pltpu.SemaphoreType.DMA((2, seqs)),
            pltpu.SemaphoreType.DMA((4, zeros + 1)),
            pltpu.SemaphoreType.DMA((2, zeros)),
            pltpu.SemaphoreType.DMA((3,)),
        ],
        compiler_params=pltpu.CompilerParams(collective_id=0, has_side_effects=True),
        name="collect",
    )(tok, cot, wgt)


def swap_kernel(give, got, send, recv):
    me_s, me_z = lax.axis_index("seq"), lax.axis_index("zero")
    sibling = (me_s // 2 * 2 + 1 - lax.rem(me_s, 2), me_z)
    greet([sibling])
    copy = remote(give.at[1], got, send, recv, sibling)
    copy.start()
    copy.wait()


def swap(split):
    return pl.pallas_call(
        swap_kernel,
        out_shape=jax.ShapeDtypeStruct(split.shape[1:], split.dtype),
        in_specs=[pl.BlockSpec(memory_space=pltpu.VMEM)],
        out_specs=pl.BlockSpec(memory_space=pltpu.VMEM),
        scratch_shapes=[pltpu.SemaphoreType.DMA, pltpu.SemaphoreType.DMA],
        compiler_params=pltpu.CompilerParams(collective_id=2, has_side_effects=True),
        name="swap",
    )(split)


def deliver_kernel(
    seqs, zeros, tok, wgt, head, tok_out, wgt_out, head_out,
    zin, zsum, tsem, zsem, wsem, hsem, loc,
):
    me_s, me_z = lax.axis_index("seq"), lax.axis_index("zero")
    every = seqs * zeros
    me = me_s * zeros + me_z
    chips = seqs // 2
    chip, core = me_s // 2, lax.rem(me_s, 2)

    def anyone(step):
        target = lax.rem(me + step, every)
        return (target // zeros, lax.rem(target, zeros))

    barrier = pltpu.get_barrier_semaphore()

    def signal(step, carry):
        pl.semaphore_signal(barrier, inc=1, device_id=anyone(step), device_id_type=MESH)
        return carry

    lax.fori_loop(1, every, signal, 0)
    pl.semaphore_wait(barrier, every - 1)

    def head_copy(step):
        return remote(head, head_out.at[me], hsem.at[0, step], hsem.at[1, step], anyone(step))

    across = []
    for d in range(1, zeros):
        target = lax.rem(me_z + d, zeros)
        across.append(
            remote(wgt.at[:, target], zin.at[d], zsem.at[0, d], zsem.at[1, d], (me_s, target))
        )
    tokens = []
    for d in range(1, chips):
        target = lax.rem(chip + d, chips)
        tokens.append(
            remote(
                tok.at[target], tok_out.at[chip], tsem.at[0, d], tsem.at[1, d],
                (target * 2 + core, me_z),
            )
        )
    own = [
        pltpu.make_async_copy(tok.at[chip], tok_out.at[chip], loc.at[0]),
        pltpu.make_async_copy(head, head_out.at[me], loc.at[1]),
    ]
    first = pltpu.make_async_copy(wgt.at[:, me_z], zin.at[0], loc.at[2])
    first.start()
    for copy in across + tokens + own:
        copy.start()
    lax.fori_loop(1, every, lambda i, c: (head_copy(i).start(), c)[1], 0)
    first.wait()
    for copy in across:
        copy.wait()

    def add(j, carry):
        total = zin[0, j].astype(F32)
        for d in range(1, zeros):
            total = total + zin[d, j].astype(F32)
        zsum[j] = total.astype(BF16)
        return carry

    lax.fori_loop(0, seqs, add, 0)
    last = pltpu.make_async_copy(zsum.at[me_s], wgt_out.at[me_s], loc.at[3])
    last.start()
    along = []
    for d in range(1, seqs):
        target = lax.rem(me_s + d, seqs)
        along.append(
            remote(
                zsum.at[target], wgt_out.at[me_s], wsem.at[0, d], wsem.at[1, d], (target, me_z)
            )
        )
    for copy in along:
        copy.start()
    for copy in own + [last] + tokens + along:
        copy.wait()
    lax.fori_loop(1, every, lambda i, c: (head_copy(i).wait(), c)[1], 0)


def deliver(tok, wgt, head, seqs, zeros):
    anywhere = pl.BlockSpec(memory_space=pl.ANY)
    every = seqs * zeros
    block = wgt.shape[2:]
    return pl.pallas_call(
        functools.partial(deliver_kernel, seqs, zeros),
        out_shape=(
            jax.ShapeDtypeStruct(tok.shape, tok.dtype),
            jax.ShapeDtypeStruct((seqs,) + block, wgt.dtype),
            jax.ShapeDtypeStruct((every,) + head.shape, head.dtype),
        ),
        in_specs=[anywhere] * 3,
        out_specs=(anywhere,) * 3,
        scratch_shapes=[
            pltpu.VMEM((zeros, seqs) + block, BF16),
            pltpu.VMEM((seqs,) + block, BF16),
            pltpu.SemaphoreType.DMA((2, seqs)),
            pltpu.SemaphoreType.DMA((2, zeros)),
            pltpu.SemaphoreType.DMA((2, seqs)),
            pltpu.SemaphoreType.DMA((2, every)),
            pltpu.SemaphoreType.DMA((4,)),
        ],
        compiler_params=pltpu.CompilerParams(collective_id=1, has_side_effects=True),
        name="deliver",
    )(tok, wgt, head)


def mixer_kernel(hp, pre_ref, dy_ref, par_ref, g_ref, split_ref, head_ref, states, grad, acc):
    chunks, inner, group = dy_ref.shape
    top = inner + 2 * STATE
    slots = acc.shape[1]
    core = lax.rem(lax.axis_index("seq"), 2)
    bias = par_ref[0][:, :1]
    rate = -jnp.exp(par_ref[1][:, :1])
    gain = par_ref[2][:, :1]
    row = lax.broadcasted_iota(jnp.int32, (group, group), 0)
    col = lax.broadcasted_iota(jnp.int32, (group, group), 1)
    causal = col >= row
    before = causal.astype(F32)
    after = (col <= row).astype(F32)

    def spread(rows):
        return jnp.concatenate(
            [jnp.broadcast_to(rows[h : h + 1], (HEAD_DIM, rows.shape[1])) for h in range(hp)], axis=0
        )

    def gather_rows(full):
        parts = [
            jnp.sum(full[h * HEAD_DIM : (h + 1) * HEAD_DIM], axis=0, keepdims=True) for h in range(hp)
        ]
        if slots > hp:
            parts.append(jnp.zeros((slots - hp, full.shape[1]), F32))
        return jnp.concatenate(parts, axis=0)

    def load(k):
        at = pl.ds(pl.multiple_of(k * group, group), group)
        pre = pre_ref[:inner, at]
        sig = jax.nn.sigmoid(pre)
        maps = pre_ref[inner:top, at]
        map_sig = jax.nn.sigmoid(maps)
        raw = pre_ref[top : top + slots, at] + bias
        step = jax.nn.softplus(raw)
        cum = exact(rate * step, before)
        return at, pre, sig, maps, map_sig, raw, step, cum

    grad[...] = jnp.zeros_like(grad)

    def forward(k, carry):
        at, pre, sig, maps, map_sig, raw, step, cum = load(k)
        last = cum[:, group - 1 :]
        x = pre * sig
        in_map = maps[:STATE] * map_sig[:STATE]
        tail = x * spread(step * jnp.exp(last - cum))
        held = grad[...]
        states[k] = held
        grad[...] = spread(jnp.exp(jnp.broadcast_to(last, (slots, STATE)))) * held + fine(nt, tail, in_map)
        return carry

    lax.fori_loop(0, chunks, forward, 0)
    grad[...] = jnp.zeros_like(grad)
    acc[...] = jnp.zeros_like(acc)

    def backward(i, carry):
        k = chunks - 1 - i
        at, pre, sig, maps, map_sig, raw, step, cum = load(k)
        last = cum[:, group - 1 :]
        x = pre * sig
        both = maps * map_sig
        in_map = both[:STATE]
        out_map = both[STATE:]
        dy16 = dy_ref[k]
        dy = dy16.astype(F32)
        u = x * spread(step)
        tail = spread(jnp.exp(last - cum))
        lead = spread(jnp.exp(cum))
        leave = spread(jnp.exp(jnp.broadcast_to(last, (slots, STATE))))
        held = states[k]
        g_out = grad[...]
        u_tail = u * tail
        dy_lead = dy * lead

        score = fine(tn, in_map, out_map)
        cum_col = jnp.concatenate([cum, jnp.zeros((group - slots, group), F32)], axis=0).T
        d_score = jnp.zeros((group, group), F32)
        ksum = jnp.zeros((group, group), F32)
        du_parts = []
        r_parts = []
        for h in range(hp):
            at_h = slice(h * HEAD_DIM, (h + 1) * HEAD_DIM)
            diff = cum[h : h + 1] - cum_col[:, h : h + 1]
            within = jnp.where(causal, jnp.exp(jnp.where(causal, diff, 0.0)), 0.0)
            mixing = score * within
            d_mix = fine(tn, u[at_h], dy16[at_h])
            du_parts.append(fine(nt, dy16[at_h], mixing))
            d_score = d_score + d_mix * within
            pair = d_mix * mixing
            r_parts.append(jnp.sum(pair, axis=0, keepdims=True))
            ksum = jnp.where(col == h, jnp.sum(pair, axis=1, keepdims=True), ksum)
        if slots > hp:
            r_parts.append(jnp.zeros((slots - hp, group), F32))
        from_tail = fine(nn, g_out, in_map) * tail
        tail_rows = gather_rows(u * from_tail)
        lead_rows = gather_rows(dy_lead * fine(nn, held, out_map))
        du = jnp.concatenate(du_parts, axis=0) + from_tail
        d_cum = jnp.concatenate(r_parts, axis=0) - ksum.T[:slots] + lead_rows - tail_rows
        cross = jnp.sum(gather_rows(held * g_out * leave) + tail_rows, axis=1, keepdims=True)
        d_log = exact(d_cum, after) + cross
        d_step = gather_rows(du * x) + rate * d_log
        d_raw = d_step * jax.nn.sigmoid(raw)

        d_out = fine(nn, in_map, d_score) + fine(tn, held, dy_lead)
        d_in = fine(nt, out_map, d_score) + fine(tn, g_out, u_tail)
        grad[...] = leave * g_out + fine(nt, dy_lead, out_map)

        slope = sig * (1.0 + pre * (1.0 - sig))
        map_slope = map_sig * (1.0 + maps * (1.0 - map_sig))
        rest = g_ref.shape[0] - top - slots
        rounded = jnp.concatenate(
            [
                (du * spread(step) + dy * gain_full) * slope,
                jnp.concatenate([d_in, d_out], axis=0) * map_slope,
                d_raw,
                jnp.zeros((rest, group), F32),
            ],
            axis=0,
        ).astype(BF16)
        g_ref[:, at] = rounded
        split_ref[lax.rem(k + core, 2), k // 2] = rounded
        acc[0] += d_raw
        acc[1] += d_log * (rate * step)
        acc[2] += gather_rows(dy * x)
        return carry

    gain_full = spread(jnp.broadcast_to(gain, (slots, group)))
    lax.fori_loop(0, chunks, backward, 0)
    for i in range(3):
        head_ref[i] = jnp.broadcast_to(jnp.sum(acc[i], axis=1, keepdims=True), head_ref.shape[1:])


def mixer(pre, dy, par, hp):
    chunks, inner, group = dy.shape
    slots = par.shape[1]
    return pl.pallas_call(
        functools.partial(mixer_kernel, hp),
        out_shape=(
            jax.ShapeDtypeStruct(pre.shape, BF16),
            jax.ShapeDtypeStruct((2, chunks // 2, pre.shape[0], group), BF16),
            jax.ShapeDtypeStruct((3, slots, 128), F32),
        ),
        in_specs=[pl.BlockSpec(memory_space=pltpu.VMEM)] * 3,
        out_specs=(pl.BlockSpec(memory_space=pltpu.VMEM),) * 3,
        scratch_shapes=[
            pltpu.VMEM((chunks, inner, STATE), F32),
            pltpu.VMEM((inner, STATE), F32),
            pltpu.VMEM((3, slots, group), F32),
        ],
        compiler_params=pltpu.CompilerParams(vmem_limit_bytes=48 * 1024 * 1024),
        name="mixer",
    )(pre, dy, par)


def body(seqs, zeros, hidden, output_grad, input_weight, step_bias, decay_log, skip_gain):
    heads = step_bias.shape[0]
    hp = up(heads, seqs) // seqs
    slots = up(hp, 8)
    inner, full = hp * HEAD_DIM, heads * HEAD_DIM
    spare = seqs * hp - heads
    width = up(inner + 2 * STATE + slots, 128)
    me = lax.axis_index("seq")
    length, model = hidden.shape[1:]

    def own(array, axis, size, extra):
        if extra:
            pads = [(0, 0)] * array.ndim
            pads[axis] = (0, extra)
            array = jnp.pad(array, pads)
        return lax.dynamic_slice_in_dim(array, me * size, size, axis)

    weight = jnp.concatenate(
        [
            own(input_weight[:, :full], 1, inner, spare * HEAD_DIM),
            input_weight[:, full : full + 2 * STATE],
            own(input_weight[:, full + 2 * STATE :], 1, hp, spare),
            jnp.zeros((input_weight.shape[0], width - inner - 2 * STATE - hp), BF16),
        ],
        axis=1,
    )
    cot = jnp.pad(output_grad[0], ((0, 0), (0, spare * HEAD_DIM))).T.reshape(seqs, inner, length)
    par = jnp.stack([own(v, 0, hp, spare) for v in (step_bias, decay_log, skip_gain)])
    par = jnp.broadcast_to(jnp.pad(par, ((0, 0), (0, slots - hp)))[:, :, None], (3, slots, 128))

    tokens, dy, columns, beside = collect(hidden[0], cot, weight, seqs, zeros)
    tokens = tokens.reshape(seqs * length, model)
    columns = columns.reshape(model, width)
    beside = beside.reshape(model, width)
    pre = lax.dot_general(columns, tokens, (((0,), (1,)), ((), ())), preferred_element_type=F32)
    grads, split, sums = mixer(pre, dy, par, hp)
    other = swap(split)

    def back(part, w):
        return lax.dot_general(part, w, (((1,), (1,)), ((), ())), preferred_element_type=F32)

    token_part = (back(split[0], columns) + back(other, beside)).astype(BF16)
    weight_part = lax.dot_general(
        tokens, grads, (((0,), (1,)), ((), ())), preferred_element_type=F32
    ).astype(BF16)
    every = seqs * zeros
    weight_part = weight_part.reshape(seqs, zeros, model // every, width)

    token_all, rows, sums_all = deliver(token_part, weight_part, sums, seqs, zeros)
    token_grad = jnp.sum(token_all.astype(F32), axis=0).astype(BF16)
    rows = rows.astype(F32)
    parts = rows.transpose(1, 0, 2)
    weight_grad = jnp.concatenate(
        [
            parts[:, :, :inner].reshape(-1, seqs * inner)[:, :full],
            jnp.sum(rows[:, :, inner : inner + 2 * STATE], axis=0),
            parts[:, :, inner + 2 * STATE : inner + 2 * STATE + hp].reshape(-1, seqs * hp)[:, :heads],
        ],
        axis=1,
    )
    sums_all = jnp.sum(sums_all.reshape(seqs, zeros, 3, slots, 128)[:, :, :, :hp, 0], axis=1)
    head_grads = sums_all.transpose(1, 0, 2).reshape(3, seqs * hp)[:, :heads]
    return (token_grad[None], weight_grad, head_grads)


def solution(mesh):
    placed = (P("zero", "seq", None), P("zero", "seq", None), P("zero", None), P(), P(), P())
    return jax.shard_map(
        functools.partial(body, mesh.shape["seq"], mesh.shape["zero"]),
        mesh=mesh,
        in_specs=placed,
        out_specs=(P("zero", "seq", None), P(("seq", "zero"), None), P()),
        check_vma=False,
    )
```

```python
import functools

import jax
import jax.numpy as jnp
from jax import lax
from jax.experimental import pallas as pl
from jax.experimental.pallas import tpu as pltpu
from jax.sharding import PartitionSpec as P

HEAD_DIM = 64
STATE = 128
MESH = pl.DeviceIdType.MESH
F32 = jnp.float32
BF16 = jnp.bfloat16


def up(size, unit):
    return -(-size // unit) * unit


def nn(a, b):
    return lax.dot_general(a, b, (((1,), (0,)), ((), ())), preferred_element_type=F32)


def nt(a, b):
    return lax.dot_general(a, b, (((1,), (1,)), ((), ())), preferred_element_type=F32)


def tn(a, b):
    return lax.dot_general(a, b, (((0,), (0,)), ((), ())), preferred_element_type=F32)


def halves(a):
    high = a.astype(BF16)
    return high, (a - high.astype(F32)).astype(BF16)


def fine(dot, a, b):
    if a.dtype == BF16:
        high, low = halves(b)
        return dot(a, high) + dot(a, low)
    if b.dtype == BF16:
        high, low = halves(a)
        return dot(high, b) + dot(low, b)
    (ah, al), (bh, bl) = halves(a), halves(b)
    return dot(ah, bh) + (dot(al, bh) + dot(ah, bl))


def exact(a, b):
    return lax.dot_general(
        a, b, (((1,), (0,)), ((), ())), precision=lax.Precision.HIGHEST, preferred_element_type=F32
    )


def greet(peers):
    barrier = pltpu.get_barrier_semaphore()
    for peer in peers:
        pl.semaphore_signal(barrier, inc=1, device_id=peer, device_id_type=MESH)
    pl.semaphore_wait(barrier, len(peers))


def remote(src, dst, send, recv, peer):
    return pltpu.make_async_remote_copy(src, dst, send, recv, peer, MESH)


def collect_kernel(
    seqs, zeros, tok, cot, wgt, tok_out, cot_out, wgt_out, wsib_out,
    tsem, fsem, csem, rsem, ssem, loc,
):
    me_s, me_z = lax.axis_index("seq"), lax.axis_index("zero")
    chips = seqs // 2
    chip, core = me_s // 2, lax.rem(me_s, 2)
    sibling = (chip * 2 + 1 - core, me_z)
    half = wgt.shape[0] // 2
    full_hops = (zeros - 1) // 2
    upper, lower = pl.ds(0, half), pl.ds(half, wgt.shape[0] - half)

    def along(step):
        return (lax.rem(me_s + step, seqs), me_z)

    def owner(shift):
        return lax.rem(me_z + shift + zeros, zeros)

    right, left = (me_s, owner(1)), (me_s, owner(-1))
    greet([along(i) for i in range(1, seqs)] + ([right, left] if zeros > 1 else []))

    own = [
        pltpu.make_async_copy(tok, tok_out.at[me_s], loc.at[0]),
        pltpu.make_async_copy(cot.at[me_s], cot_out.at[me_s], loc.at[1]),
        pltpu.make_async_copy(wgt, wgt_out.at[me_z], loc.at[2]),
    ]

    def hop(way, h):
        at = owner(-way * (h - 1))
        src = wgt if h == 1 else wgt_out.at[at]
        dst = wgt_out.at[at]
        if h > full_hops:
            rows = upper if way > 0 else lower
            src, dst = src.at[rows], dst.at[rows]
        row = 0 if way > 0 else 2
        return remote(src, dst, rsem.at[row, h], rsem.at[row + 1, h], right if way > 0 else left)

    hops = full_hops + (1 - zeros % 2)
    ring = [(hop(1, h), hop(-1, h)) for h in range(1, hops + 1)]

    def token_slot(step):
        return lax.rem(chip - step + chips, chips) * 2 + core

    tokens = [
        remote(
            tok, tok_out.at[me_s], tsem.at[0, d], tsem.at[1, d],
            (lax.rem(chip + d, chips) * 2 + core, me_z),
        )
        for d in range(1, chips)
    ]
    cots = []
    for d in range(1, seqs):
        peer = along(d)
        cots.append(
            remote(cot.at[peer[0]], cot_out.at[me_s], csem.at[0, d], csem.at[1, d], peer)
        )
    passed = [remote(tok, tok_out.at[me_s], fsem.at[0, 0], fsem.at[1, 0], sibling)]
    for d in range(1, chips):
        at = token_slot(d)
        passed.append(remote(tok_out.at[at], tok_out.at[at], fsem.at[0, d], fsem.at[1, d], sibling))

    def share(slot, at, src):
        return remote(src, wsib_out.at[at], ssem.at[0, slot], ssem.at[1, slot], sibling)

    shared = [share(0, me_z, wgt)]
    for d in range(1, zeros):
        at = owner(-d)
        shared.append(share(d, at, wgt_out.at[at]))

    for copy in ring[0] if ring else ():
        copy.start()
    for copy in tokens + cots + [passed[0], shared[0]] + own:
        copy.start()
    for h in range(1, hops):
        for way in (0, 1):
            ring[h - 1][way].wait_recv()
            ring[h][way].start()
    for d in range(1, chips):
        tokens[d - 1].wait_recv()
        passed[d].start()
    if ring:
        for way in (0, 1):
            ring[-1][way].wait_recv()
    for copy in shared[1:]:
        copy.start()
    for pair in ring:
        for copy in pair:
            copy.wait_send()
    for copy in tokens:
        copy.wait_send()
    for copy in own + cots + passed + shared:
        copy.wait()


def collect(tok, cot, wgt, seqs, zeros):
    anywhere = pl.BlockSpec(memory_space=pl.ANY)
    columns = jax.ShapeDtypeStruct((zeros,) + wgt.shape, wgt.dtype)
    return pl.pallas_call(
        functools.partial(collect_kernel, seqs, zeros),
        out_shape=(
            jax.ShapeDtypeStruct((seqs,) + tok.shape, tok.dtype),
            jax.ShapeDtypeStruct(cot.shape, cot.dtype),
            columns,
            columns,
        ),
        in_specs=[anywhere] * 3,
        out_specs=(anywhere,) * 4,
        scratch_shapes=[
            pltpu.SemaphoreType.DMA((2, seqs)),
            pltpu.SemaphoreType.DMA((2, seqs)),
            pltpu.SemaphoreType.DMA((2, seqs)),
            pltpu.SemaphoreType.DMA((4, zeros + 1)),
            pltpu.SemaphoreType.DMA((2, zeros)),
            pltpu.SemaphoreType.DMA((3,)),
        ],
        compiler_params=pltpu.CompilerParams(collective_id=0, has_side_effects=True),
        name="collect",
    )(tok, cot, wgt)


def swap_kernel(give, maps, got, got_map, send, recv):
    me_s, me_z = lax.axis_index("seq"), lax.axis_index("zero")
    core = lax.rem(me_s, 2)
    sibling = (me_s // 2 * 2 + 1 - core, me_z)
    greet([sibling])
    copies = [
        remote(maps.at[1 - core], got_map, send.at[0], recv.at[0], sibling),
        remote(give.at[1], got, send.at[1], recv.at[1], sibling),
    ]
    for copy in copies:
        copy.start()
    for copy in copies:
        copy.wait()


def swap(split, maps):
    vmem = pl.BlockSpec(memory_space=pltpu.VMEM)
    return pl.pallas_call(
        swap_kernel,
        out_shape=(
            jax.ShapeDtypeStruct(split.shape[1:], split.dtype),
            jax.ShapeDtypeStruct(maps.shape[1:], maps.dtype),
        ),
        in_specs=[vmem, vmem],
        out_specs=(vmem, vmem),
        scratch_shapes=[pltpu.SemaphoreType.DMA((2,)), pltpu.SemaphoreType.DMA((2,))],
        compiler_params=pltpu.CompilerParams(collective_id=2, has_side_effects=True),
        name="swap",
    )(split, maps)


def deliver_kernel(
    seqs, zeros, tok, wgt, head, tok_out, wgt_out, head_out,
    zin, zsum, tsem, zsem, wsem, hsem, loc,
):
    me_s, me_z = lax.axis_index("seq"), lax.axis_index("zero")
    every = seqs * zeros
    me = me_s * zeros + me_z
    chips = seqs // 2
    chip, core = me_s // 2, lax.rem(me_s, 2)

    def anyone(step):
        target = lax.rem(me + step, every)
        return (target // zeros, lax.rem(target, zeros))

    barrier = pltpu.get_barrier_semaphore()

    def signal(step, carry):
        pl.semaphore_signal(barrier, inc=1, device_id=anyone(step), device_id_type=MESH)
        return carry

    lax.fori_loop(1, every, signal, 0)
    pl.semaphore_wait(barrier, every - 1)

    def head_copy(step):
        return remote(head, head_out.at[me], hsem.at[0, step], hsem.at[1, step], anyone(step))

    across = []
    for d in range(1, zeros):
        target = lax.rem(me_z + d, zeros)
        across.append(
            remote(wgt.at[:, target], zin.at[d], zsem.at[0, d], zsem.at[1, d], (me_s, target))
        )
    tokens = []
    for d in range(1, chips):
        target = lax.rem(chip + d, chips)
        tokens.append(
            remote(
                tok.at[target], tok_out.at[chip], tsem.at[0, d], tsem.at[1, d],
                (target * 2 + core, me_z),
            )
        )
    own = [
        pltpu.make_async_copy(tok.at[chip], tok_out.at[chip], loc.at[0]),
        pltpu.make_async_copy(head, head_out.at[me], loc.at[1]),
    ]
    first = pltpu.make_async_copy(wgt.at[:, me_z], zin.at[0], loc.at[2])
    first.start()
    for copy in across + tokens + own:
        copy.start()
    lax.fori_loop(1, every, lambda i, c: (head_copy(i).start(), c)[1], 0)
    first.wait()
    for copy in across:
        copy.wait()

    def add(j, carry):
        total = zin[0, j].astype(F32)
        for d in range(1, zeros):
            total = total + zin[d, j].astype(F32)
        zsum[j] = total.astype(BF16)
        return carry

    lax.fori_loop(0, seqs, add, 0)
    last = pltpu.make_async_copy(zsum.at[me_s], wgt_out.at[me_s], loc.at[3])
    last.start()
    along = []
    for d in range(1, seqs):
        target = lax.rem(me_s + d, seqs)
        along.append(
            remote(
                zsum.at[target], wgt_out.at[me_s], wsem.at[0, d], wsem.at[1, d], (target, me_z)
            )
        )
    for copy in along:
        copy.start()
    for copy in own + [last] + tokens + along:
        copy.wait()
    lax.fori_loop(1, every, lambda i, c: (head_copy(i).wait(), c)[1], 0)


def deliver(tok, wgt, head, seqs, zeros):
    anywhere = pl.BlockSpec(memory_space=pl.ANY)
    every = seqs * zeros
    block = wgt.shape[2:]
    return pl.pallas_call(
        functools.partial(deliver_kernel, seqs, zeros),
        out_shape=(
            jax.ShapeDtypeStruct(tok.shape, tok.dtype),
            jax.ShapeDtypeStruct((seqs,) + block, wgt.dtype),
            jax.ShapeDtypeStruct((every,) + head.shape, head.dtype),
        ),
        in_specs=[anywhere] * 3,
        out_specs=(anywhere,) * 3,
        scratch_shapes=[
            pltpu.VMEM((zeros, seqs) + block, BF16),
            pltpu.VMEM((seqs,) + block, BF16),
            pltpu.SemaphoreType.DMA((2, seqs)),
            pltpu.SemaphoreType.DMA((2, zeros)),
            pltpu.SemaphoreType.DMA((2, seqs)),
            pltpu.SemaphoreType.DMA((2, every)),
            pltpu.SemaphoreType.DMA((4,)),
        ],
        compiler_params=pltpu.CompilerParams(collective_id=1, has_side_effects=True),
        name="deliver",
    )(tok, wgt, head)


def mixer_kernel(hp, pre_ref, dy_ref, par_ref, g_ref, split_ref, maps_ref, head_ref, states, grad, acc):
    chunks, inner, group = dy_ref.shape
    top = inner + 2 * STATE
    slots = acc.shape[1]
    core = lax.rem(lax.axis_index("seq"), 2)
    bias = par_ref[0][:, :1]
    rate = -jnp.exp(par_ref[1][:, :1])
    gain = par_ref[2][:, :1]
    row = lax.broadcasted_iota(jnp.int32, (group, group), 0)
    col = lax.broadcasted_iota(jnp.int32, (group, group), 1)
    causal = col >= row
    before = causal.astype(F32)
    after = (col <= row).astype(F32)

    def spread(rows):
        return jnp.concatenate(
            [jnp.broadcast_to(rows[h : h + 1], (HEAD_DIM, rows.shape[1])) for h in range(hp)], axis=0
        )

    def gather_rows(full):
        parts = [
            jnp.sum(full[h * HEAD_DIM : (h + 1) * HEAD_DIM], axis=0, keepdims=True) for h in range(hp)
        ]
        if slots > hp:
            parts.append(jnp.zeros((slots - hp, full.shape[1]), F32))
        return jnp.concatenate(parts, axis=0)

    def load(k):
        at = pl.ds(pl.multiple_of(k * group, group), group)
        pre = pre_ref[:inner, at]
        sig = jax.nn.sigmoid(pre)
        maps = pre_ref[inner:top, at]
        map_sig = jax.nn.sigmoid(maps)
        raw = pre_ref[top : top + slots, at] + bias
        step = jax.nn.softplus(raw)
        cum = exact(rate * step, before)
        return at, pre, sig, maps, map_sig, raw, step, cum

    grad[...] = jnp.zeros_like(grad)

    def forward(k, carry):
        at, pre, sig, maps, map_sig, raw, step, cum = load(k)
        last = cum[:, group - 1 :]
        x = pre * sig
        in_map = maps[:STATE] * map_sig[:STATE]
        tail = x * spread(step * jnp.exp(last - cum))
        held = grad[...]
        states[k] = held
        grad[...] = spread(jnp.exp(jnp.broadcast_to(last, (slots, STATE)))) * held + fine(nt, tail, in_map)
        return carry

    lax.fori_loop(0, chunks, forward, 0)
    grad[...] = jnp.zeros_like(grad)
    acc[...] = jnp.zeros_like(acc)

    def backward(i, carry):
        k = chunks - 1 - i
        at, pre, sig, maps, map_sig, raw, step, cum = load(k)
        last = cum[:, group - 1 :]
        x = pre * sig
        both = maps * map_sig
        in_map = both[:STATE]
        out_map = both[STATE:]
        dy16 = dy_ref[k]
        dy = dy16.astype(F32)
        u = x * spread(step)
        tail = spread(jnp.exp(last - cum))
        lead = spread(jnp.exp(cum))
        leave = spread(jnp.exp(jnp.broadcast_to(last, (slots, STATE))))
        held = states[k]
        g_out = grad[...]
        u_tail = u * tail
        dy_lead = dy * lead

        score = fine(tn, in_map, out_map)
        cum_col = jnp.concatenate([cum, jnp.zeros((group - slots, group), F32)], axis=0).T
        d_score = jnp.zeros((group, group), F32)
        ksum = jnp.zeros((group, group), F32)
        du_parts = []
        r_parts = []
        for h in range(hp):
            at_h = slice(h * HEAD_DIM, (h + 1) * HEAD_DIM)
            diff = cum[h : h + 1] - cum_col[:, h : h + 1]
            within = jnp.where(causal, jnp.exp(jnp.where(causal, diff, 0.0)), 0.0)
            mixing = score * within
            d_mix = fine(tn, u[at_h], dy16[at_h])
            du_parts.append(fine(nt, dy16[at_h], mixing))
            d_score = d_score + d_mix * within
            pair = d_mix * mixing
            r_parts.append(jnp.sum(pair, axis=0, keepdims=True))
            ksum = jnp.where(col == h, jnp.sum(pair, axis=1, keepdims=True), ksum)
        if slots > hp:
            r_parts.append(jnp.zeros((slots - hp, group), F32))
        from_tail = fine(nn, g_out, in_map) * tail
        tail_rows = gather_rows(u * from_tail)
        lead_rows = gather_rows(dy_lead * fine(nn, held, out_map))
        du = jnp.concatenate(du_parts, axis=0) + from_tail
        d_cum = jnp.concatenate(r_parts, axis=0) - ksum.T[:slots] + lead_rows - tail_rows
        cross = jnp.sum(gather_rows(held * g_out * leave) + tail_rows, axis=1, keepdims=True)
        d_log = exact(d_cum, after) + cross
        d_step = gather_rows(du * x) + rate * d_log
        d_raw = d_step * jax.nn.sigmoid(raw)

        d_out = fine(nn, in_map, d_score) + fine(tn, held, dy_lead)
        d_in = fine(nt, out_map, d_score) + fine(tn, g_out, u_tail)
        grad[...] = leave * g_out + fine(nt, dy_lead, out_map)

        slope = sig * (1.0 + pre * (1.0 - sig))
        map_slope = map_sig * (1.0 + maps * (1.0 - map_sig))
        rest = g_ref.shape[0] - inner - STATE - slots
        rounded = jnp.concatenate(
            [
                (du * spread(step) + dy * gain_full) * slope,
                jnp.concatenate([d_in, d_out], axis=0) * map_slope,
                d_raw,
                jnp.zeros((rest, group), F32),
            ],
            axis=0,
        ).astype(BF16)
        maps_ref[0, :, at] = d_in * map_slope[:STATE]
        maps_ref[1, :, at] = d_out * map_slope[STATE:]
        g_ref[:inner, at] = rounded[:inner]
        g_ref[inner : inner + STATE, at] = jnp.zeros((STATE, group), BF16)
        g_ref[inner + STATE :, at] = rounded[top:]
        split_ref[lax.rem(k + core, 2), k // 2] = rounded
        acc[0] += d_raw
        acc[1] += d_log * (rate * step)
        acc[2] += gather_rows(dy * x)
        return carry

    gain_full = spread(jnp.broadcast_to(gain, (slots, group)))
    lax.fori_loop(0, chunks, backward, 0)
    for i in range(3):
        head_ref[i] = jnp.broadcast_to(jnp.sum(acc[i], axis=1, keepdims=True), head_ref.shape[1:])


def mixer(pre, dy, par, hp):
    chunks, inner, group = dy.shape
    slots = par.shape[1]
    return pl.pallas_call(
        functools.partial(mixer_kernel, hp),
        out_shape=(
            jax.ShapeDtypeStruct((pre.shape[0] - STATE, pre.shape[1]), BF16),
            jax.ShapeDtypeStruct((2, chunks // 2, pre.shape[0], group), BF16),
            jax.ShapeDtypeStruct((2, STATE, pre.shape[1]), F32),
            jax.ShapeDtypeStruct((3, slots, 128), F32),
        ),
        in_specs=[pl.BlockSpec(memory_space=pltpu.VMEM)] * 3,
        out_specs=(pl.BlockSpec(memory_space=pltpu.VMEM),) * 4,
        scratch_shapes=[
            pltpu.VMEM((chunks, inner, STATE), F32),
            pltpu.VMEM((inner, STATE), F32),
            pltpu.VMEM((3, slots, group), F32),
        ],
        compiler_params=pltpu.CompilerParams(vmem_limit_bytes=48 * 1024 * 1024),
        name="mixer",
    )(pre, dy, par)


def body(seqs, zeros, hidden, output_grad, input_weight, step_bias, decay_log, skip_gain):
    heads = step_bias.shape[0]
    hp = up(heads, seqs) // seqs
    slots = up(hp, 8)
    inner, full = hp * HEAD_DIM, heads * HEAD_DIM
    spare = seqs * hp - heads
    width = up(inner + STATE + slots, 128)
    me = lax.axis_index("seq")
    core = lax.rem(me, 2)
    mine = inner + STATE
    length, model = hidden.shape[1:]

    def own(array, axis, size, extra):
        if extra:
            pads = [(0, 0)] * array.ndim
            pads[axis] = (0, extra)
            array = jnp.pad(array, pads)
        return lax.dynamic_slice_in_dim(array, me * size, size, axis)

    weight = jnp.concatenate(
        [
            own(input_weight[:, :full], 1, inner, spare * HEAD_DIM),
            lax.dynamic_slice_in_dim(input_weight[:, full : full + 2 * STATE], core * STATE, STATE, 1),
            own(input_weight[:, full + 2 * STATE :], 1, hp, spare),
            jnp.zeros((input_weight.shape[0], width - mine - hp), BF16),
        ],
        axis=1,
    )
    cot = jnp.pad(output_grad[0], ((0, 0), (0, spare * HEAD_DIM))).T.reshape(seqs, inner, length)
    par = jnp.stack([own(v, 0, hp, spare) for v in (step_bias, decay_log, skip_gain)])
    par = jnp.broadcast_to(jnp.pad(par, ((0, 0), (0, slots - hp)))[:, :, None], (3, slots, 128))

    tokens, dy, columns, beside = collect(hidden[0], cot, weight, seqs, zeros)
    tokens = tokens.reshape(seqs * length, model)
    columns = columns.reshape(model, width)
    beside = beside.reshape(model, width)
    here, there = columns[:, inner:mine], beside[:, inner:mine]
    both = [jnp.where(core == 0, here, there), jnp.where(core == 0, there, here)]
    columns = jnp.concatenate([columns[:, :inner]] + both + [columns[:, mine:]], axis=1)
    beside = jnp.concatenate([beside[:, :inner]] + both + [beside[:, mine:]], axis=1)
    pre = lax.dot_general(columns, tokens, (((0,), (1,)), ((), ())), preferred_element_type=F32)
    grads, split, maps, sums = mixer(pre, dy, par, hp)
    other, other_map = swap(split, maps)
    pair_map = lax.dynamic_index_in_dim(maps, core, 0, False) + other_map
    grads = jnp.concatenate([grads[:inner], pair_map.astype(BF16), grads[mine:]], axis=0)

    def back(part, w):
        return lax.dot_general(part, w, (((1,), (1,)), ((), ())), preferred_element_type=F32)

    token_part = (back(split[0], columns) + back(other, beside)).astype(BF16)
    weight_part = lax.dot_general(
        tokens, grads, (((0,), (1,)), ((), ())), preferred_element_type=F32
    ).astype(BF16)
    every = seqs * zeros
    weight_part = weight_part.reshape(seqs, zeros, model // every, width)

    token_all, rows, sums_all = deliver(token_part, weight_part, sums, seqs, zeros)
    token_grad = jnp.sum(token_all.astype(F32), axis=0).astype(BF16)
    rows = rows.astype(F32)
    parts = rows.transpose(1, 0, 2)
    weight_grad = jnp.concatenate(
        [
            parts[:, :, :inner].reshape(-1, seqs * inner)[:, :full],
            jnp.sum(rows[0::2, :, inner:mine], axis=0),
            jnp.sum(rows[1::2, :, inner:mine], axis=0),
            parts[:, :, mine : mine + hp].reshape(-1, seqs * hp)[:, :heads],
        ],
        axis=1,
    )
    sums_all = jnp.sum(sums_all.reshape(seqs, zeros, 3, slots, 128)[:, :, :, :hp, 0], axis=1)
    head_grads = sums_all.transpose(1, 0, 2).reshape(3, seqs * hp)[:, :heads]
    return (token_grad[None], weight_grad, head_grads)


def solution(mesh):
    placed = (P("zero", "seq", None), P("zero", "seq", None), P("zero", None), P(), P(), P())
    return jax.shard_map(
        functools.partial(body, mesh.shape["seq"], mesh.shape["zero"]),
        mesh=mesh,
        in_specs=placed,
        out_specs=(P("zero", "seq", None), P(("seq", "zero"), None), P()),
        check_vma=False,
    )
```

```python
import functools

import jax
import jax.numpy as jnp
from jax import lax
from jax.experimental import pallas as pl
from jax.experimental.pallas import tpu as pltpu
from jax.sharding import PartitionSpec as P

HEAD_DIM = 64
STATE = 128
MESH = pl.DeviceIdType.MESH
F32 = jnp.float32
BF16 = jnp.bfloat16


def up(size, unit):
    return -(-size // unit) * unit


def nn(a, b):
    return lax.dot_general(a, b, (((1,), (0,)), ((), ())), preferred_element_type=F32)


def nt(a, b):
    return lax.dot_general(a, b, (((1,), (1,)), ((), ())), preferred_element_type=F32)


def tn(a, b):
    return lax.dot_general(a, b, (((0,), (0,)), ((), ())), preferred_element_type=F32)


def halves(a):
    high = a.astype(BF16)
    return high, (a - high.astype(F32)).astype(BF16)


def fine(dot, a, b):
    if a.dtype == BF16:
        high, low = halves(b)
        return dot(a, high) + dot(a, low)
    if b.dtype == BF16:
        high, low = halves(a)
        return dot(high, b) + dot(low, b)
    (ah, al), (bh, bl) = halves(a), halves(b)
    return dot(ah, bh) + (dot(al, bh) + dot(ah, bl))


def exact(a, b):
    return lax.dot_general(
        a, b, (((1,), (0,)), ((), ())), precision=lax.Precision.HIGHEST, preferred_element_type=F32
    )


def greet(peers):
    barrier = pltpu.get_barrier_semaphore()
    for peer in peers:
        pl.semaphore_signal(barrier, inc=1, device_id=peer, device_id_type=MESH)
    pl.semaphore_wait(barrier, len(peers))


def remote(src, dst, send, recv, peer):
    return pltpu.make_async_remote_copy(src, dst, send, recv, peer, MESH)


def collect_kernel(
    seqs, zeros, tok, cot, wgt, tok_out, cot_out, wgt_out, wsib_out,
    tsem, fsem, csem, rsem, ssem, loc,
):
    me_s, me_z = lax.axis_index("seq"), lax.axis_index("zero")
    chips = seqs // 2
    chip, core = me_s // 2, lax.rem(me_s, 2)
    sibling = (chip * 2 + 1 - core, me_z)
    half = wgt.shape[0] // 2
    full_hops = (zeros - 1) // 2
    upper, lower = pl.ds(0, half), pl.ds(half, wgt.shape[0] - half)

    def along(step):
        return (lax.rem(me_s + step, seqs), me_z)

    def owner(shift):
        return lax.rem(me_z + shift + zeros, zeros)

    right, left = (me_s, owner(1)), (me_s, owner(-1))
    greet([along(i) for i in range(1, seqs)] + ([right, left] if zeros > 1 else []))

    own = [
        pltpu.make_async_copy(tok, tok_out.at[me_s], loc.at[0]),
        pltpu.make_async_copy(cot.at[me_s], cot_out.at[me_s], loc.at[1]),
        pltpu.make_async_copy(wgt, wgt_out.at[me_z], loc.at[2]),
    ]

    def hop(way, h):
        at = owner(-way * (h - 1))
        src = wgt if h == 1 else wgt_out.at[at]
        dst = wgt_out.at[at]
        if h > full_hops:
            rows = upper if way > 0 else lower
            src, dst = src.at[rows], dst.at[rows]
        row = 0 if way > 0 else 2
        return remote(src, dst, rsem.at[row, h], rsem.at[row + 1, h], right if way > 0 else left)

    hops = full_hops + (1 - zeros % 2)
    ring = [(hop(1, h), hop(-1, h)) for h in range(1, hops + 1)]

    def token_slot(step):
        return lax.rem(chip - step + chips, chips) * 2 + core

    tokens = [
        remote(
            tok, tok_out.at[me_s], tsem.at[0, d], tsem.at[1, d],
            (lax.rem(chip + d, chips) * 2 + core, me_z),
        )
        for d in range(1, chips)
    ]
    cots = []
    for d in range(1, seqs):
        peer = along(d)
        cots.append(
            remote(cot.at[peer[0]], cot_out.at[me_s], csem.at[0, d], csem.at[1, d], peer)
        )
    passed = [remote(tok, tok_out.at[me_s], fsem.at[0, 0], fsem.at[1, 0], sibling)]
    for d in range(1, chips):
        at = token_slot(d)
        passed.append(remote(tok_out.at[at], tok_out.at[at], fsem.at[0, d], fsem.at[1, d], sibling))

    def share(slot, at, src):
        return remote(src, wsib_out.at[at], ssem.at[0, slot], ssem.at[1, slot], sibling)

    shared = [share(0, me_z, wgt)]
    for d in range(1, zeros):
        at = owner(-d)
        shared.append(share(d, at, wgt_out.at[at]))

    for copy in ring[0] if ring else ():
        copy.start()
    for copy in tokens + cots + [passed[0], shared[0]] + own:
        copy.start()
    for h in range(1, hops):
        for way in (0, 1):
            ring[h - 1][way].wait_recv()
            ring[h][way].start()
    for d in range(1, chips):
        tokens[d - 1].wait_recv()
        passed[d].start()
    if ring:
        for way in (0, 1):
            ring[-1][way].wait_recv()
    for copy in shared[1:]:
        copy.start()
    for pair in ring:
        for copy in pair:
            copy.wait_send()
    for copy in tokens:
        copy.wait_send()
    for copy in own + cots + passed + shared:
        copy.wait()


def collect(tok, cot, wgt, seqs, zeros):
    anywhere = pl.BlockSpec(memory_space=pl.ANY)
    columns = jax.ShapeDtypeStruct((zeros,) + wgt.shape, wgt.dtype)
    return pl.pallas_call(
        functools.partial(collect_kernel, seqs, zeros),
        out_shape=(
            jax.ShapeDtypeStruct((seqs,) + tok.shape, tok.dtype),
            jax.ShapeDtypeStruct(cot.shape, cot.dtype),
            columns,
            columns,
        ),
        in_specs=[anywhere] * 3,
        out_specs=(anywhere,) * 4,
        scratch_shapes=[
            pltpu.SemaphoreType.DMA((2, seqs)),
            pltpu.SemaphoreType.DMA((2, seqs)),
            pltpu.SemaphoreType.DMA((2, seqs)),
            pltpu.SemaphoreType.DMA((4, zeros + 1)),
            pltpu.SemaphoreType.DMA((2, zeros)),
            pltpu.SemaphoreType.DMA((3,)),
        ],
        compiler_params=pltpu.CompilerParams(collective_id=0, has_side_effects=True),
        name="collect",
    )(tok, cot, wgt)


def swap_kernel(give, maps, got, got_map, send, recv):
    me_s, me_z = lax.axis_index("seq"), lax.axis_index("zero")
    core = lax.rem(me_s, 2)
    sibling = (me_s // 2 * 2 + 1 - core, me_z)
    greet([sibling])
    copies = [
        remote(maps.at[1 - core], got_map, send.at[0], recv.at[0], sibling),
        remote(give.at[1], got, send.at[1], recv.at[1], sibling),
    ]
    for copy in copies:
        copy.start()
    for copy in copies:
        copy.wait()


def swap(split, maps):
    anywhere = pl.BlockSpec(memory_space=pl.ANY)
    return pl.pallas_call(
        swap_kernel,
        out_shape=(
            jax.ShapeDtypeStruct(split.shape[1:], split.dtype),
            jax.ShapeDtypeStruct(maps.shape[1:], maps.dtype),
        ),
        in_specs=[anywhere, anywhere],
        out_specs=(anywhere, anywhere),
        scratch_shapes=[pltpu.SemaphoreType.DMA((2,)), pltpu.SemaphoreType.DMA((2,))],
        compiler_params=pltpu.CompilerParams(collective_id=2, has_side_effects=True),
        name="swap",
    )(split, maps)


def deliver_kernel(
    seqs, zeros, tok, wgt, head, tok_out, wgt_out, head_out,
    zin, zsum, hin, hsum, tsem, zsem, wsem, hsem, gsem, loc,
):
    me_s, me_z = lax.axis_index("seq"), lax.axis_index("zero")
    chips = seqs // 2
    chip, core = me_s // 2, lax.rem(me_s, 2)
    greet(
        [(me_s, lax.rem(me_z + d, zeros)) for d in range(1, zeros)]
        + [(lax.rem(me_s + d, seqs), me_z) for d in range(1, seqs)]
    )
    across = []
    for d in range(1, zeros):
        target = lax.rem(me_z + d, zeros)
        across.append(
            remote(wgt.at[:, target], zin.at[d], zsem.at[0, d], zsem.at[1, d], (me_s, target))
        )
        across.append(remote(head, hin.at[d], hsem.at[0, d], hsem.at[1, d], (me_s, target)))
    tokens = []
    for d in range(1, chips):
        target = lax.rem(chip + d, chips)
        tokens.append(
            remote(
                tok.at[target], tok_out.at[chip], tsem.at[0, d], tsem.at[1, d],
                (target * 2 + core, me_z),
            )
        )
    own = [pltpu.make_async_copy(tok.at[chip], tok_out.at[chip], loc.at[0])]
    first = [
        pltpu.make_async_copy(wgt.at[:, me_z], zin.at[0], loc.at[2]),
        pltpu.make_async_copy(head, hin.at[0], loc.at[1]),
    ]
    for copy in across + tokens + first + own:
        copy.start()
    for copy in first + across:
        copy.wait()
    sums = hin[0]
    for d in range(1, zeros):
        sums = sums + hin[d]
    hsum[...] = sums

    def add(j, carry):
        total = zin[0, j].astype(F32)
        for d in range(1, zeros):
            total = total + zin[d, j].astype(F32)
        zsum[j] = total.astype(BF16)
        return carry

    lax.fori_loop(0, seqs, add, 0)
    own += [
        pltpu.make_async_copy(zsum.at[me_s], wgt_out.at[me_s], loc.at[3]),
        pltpu.make_async_copy(hsum, head_out.at[me_s], loc.at[4]),
    ]
    for copy in own[1:]:
        copy.start()
    along = []
    for d in range(1, seqs):
        target = lax.rem(me_s + d, seqs)
        along.append(
            remote(
                zsum.at[target], wgt_out.at[me_s], wsem.at[0, d], wsem.at[1, d], (target, me_z)
            )
        )
        along.append(
            remote(hsum, head_out.at[me_s], gsem.at[0, d], gsem.at[1, d], (target, me_z))
        )
    for copy in along:
        copy.start()
    for copy in own + tokens + along:
        copy.wait()


def deliver(tok, wgt, head, seqs, zeros):
    anywhere = pl.BlockSpec(memory_space=pl.ANY)
    block = wgt.shape[2:]
    return pl.pallas_call(
        functools.partial(deliver_kernel, seqs, zeros),
        out_shape=(
            jax.ShapeDtypeStruct(tok.shape, tok.dtype),
            jax.ShapeDtypeStruct((seqs,) + block, wgt.dtype),
            jax.ShapeDtypeStruct((seqs,) + head.shape, head.dtype),
        ),
        in_specs=[anywhere] * 3,
        out_specs=(anywhere,) * 3,
        scratch_shapes=[
            pltpu.VMEM((zeros, seqs) + block, BF16),
            pltpu.VMEM((seqs,) + block, BF16),
            pltpu.VMEM((zeros,) + head.shape, F32),
            pltpu.VMEM(head.shape, F32),
            pltpu.SemaphoreType.DMA((2, seqs)),
            pltpu.SemaphoreType.DMA((2, zeros)),
            pltpu.SemaphoreType.DMA((2, seqs)),
            pltpu.SemaphoreType.DMA((2, zeros)),
            pltpu.SemaphoreType.DMA((2, seqs)),
            pltpu.SemaphoreType.DMA((5,)),
        ],
        compiler_params=pltpu.CompilerParams(collective_id=1, has_side_effects=True),
        name="deliver",
    )(tok, wgt, head)


def mixer_kernel(hp, pre_ref, dy_ref, par_ref, g_ref, split_ref, maps_ref, head_ref, states, grad, acc):
    chunks, inner, group = dy_ref.shape
    top = inner + 2 * STATE
    slots = acc.shape[1]
    core = lax.rem(lax.axis_index("seq"), 2)
    bias = par_ref[0][:, :1]
    rate = -jnp.exp(par_ref[1][:, :1])
    gain = par_ref[2][:, :1]
    row = lax.broadcasted_iota(jnp.int32, (group, group), 0)
    col = lax.broadcasted_iota(jnp.int32, (group, group), 1)
    causal = col >= row
    before = causal.astype(F32)
    after = (col <= row).astype(F32)

    def spread(rows):
        return jnp.concatenate(
            [jnp.broadcast_to(rows[h : h + 1], (HEAD_DIM, rows.shape[1])) for h in range(hp)], axis=0
        )

    def gather_rows(full):
        parts = [
            jnp.sum(full[h * HEAD_DIM : (h + 1) * HEAD_DIM], axis=0, keepdims=True) for h in range(hp)
        ]
        if slots > hp:
            parts.append(jnp.zeros((slots - hp, full.shape[1]), F32))
        return jnp.concatenate(parts, axis=0)

    def load(k):
        at = pl.ds(pl.multiple_of(k * group, group), group)
        pre = pre_ref[:inner, at]
        sig = jax.nn.sigmoid(pre)
        maps = pre_ref[inner:top, at]
        map_sig = jax.nn.sigmoid(maps)
        raw = pre_ref[top : top + slots, at] + bias
        step = jax.nn.softplus(raw)
        cum = exact(rate * step, before)
        return at, pre, sig, maps, map_sig, raw, step, cum

    grad[...] = jnp.zeros_like(grad)

    def forward(k, carry):
        at, pre, sig, maps, map_sig, raw, step, cum = load(k)
        last = cum[:, group - 1 :]
        x = pre * sig
        in_map = maps[:STATE] * map_sig[:STATE]
        tail = x * spread(step * jnp.exp(last - cum))
        held = grad[...]
        states[k] = held
        grad[...] = spread(jnp.exp(jnp.broadcast_to(last, (slots, STATE)))) * held + fine(nt, tail, in_map)
        return carry

    lax.fori_loop(0, chunks, forward, 0)
    grad[...] = jnp.zeros_like(grad)
    acc[...] = jnp.zeros_like(acc)

    def backward(i, carry):
        k = chunks - 1 - i
        at, pre, sig, maps, map_sig, raw, step, cum = load(k)
        last = cum[:, group - 1 :]
        x = pre * sig
        both = maps * map_sig
        in_map = both[:STATE]
        out_map = both[STATE:]
        dy16 = dy_ref[k]
        dy = dy16.astype(F32)
        u = x * spread(step)
        tail = spread(jnp.exp(last - cum))
        lead = spread(jnp.exp(cum))
        leave = spread(jnp.exp(jnp.broadcast_to(last, (slots, STATE))))
        held = states[k]
        g_out = grad[...]
        u_tail = u * tail
        dy_lead = dy * lead

        score = fine(tn, in_map, out_map)
        cum_col = jnp.concatenate([cum, jnp.zeros((group - slots, group), F32)], axis=0).T
        d_score = jnp.zeros((group, group), F32)
        ksum = jnp.zeros((group, group), F32)
        du_parts = []
        r_parts = []
        for h in range(hp):
            at_h = slice(h * HEAD_DIM, (h + 1) * HEAD_DIM)
            diff = cum[h : h + 1] - cum_col[:, h : h + 1]
            within = jnp.where(causal, jnp.exp(jnp.where(causal, diff, 0.0)), 0.0)
            mixing = score * within
            d_mix = fine(tn, u[at_h], dy16[at_h])
            du_parts.append(fine(nt, dy16[at_h], mixing))
            d_score = d_score + d_mix * within
            pair = d_mix * mixing
            r_parts.append(jnp.sum(pair, axis=0, keepdims=True))
            ksum = jnp.where(col == h, jnp.sum(pair, axis=1, keepdims=True), ksum)
        if slots > hp:
            r_parts.append(jnp.zeros((slots - hp, group), F32))
        from_tail = fine(nn, g_out, in_map) * tail
        tail_rows = gather_rows(u * from_tail)
        lead_rows = gather_rows(dy_lead * fine(nn, held, out_map))
        du = jnp.concatenate(du_parts, axis=0) + from_tail
        d_cum = jnp.concatenate(r_parts, axis=0) - ksum.T[:slots] + lead_rows - tail_rows
        cross = jnp.sum(gather_rows(held * g_out * leave) + tail_rows, axis=1, keepdims=True)
        d_log = exact(d_cum, after) + cross
        d_step = gather_rows(du * x) + rate * d_log
        d_raw = d_step * jax.nn.sigmoid(raw)

        d_out = fine(nn, in_map, d_score) + fine(tn, held, dy_lead)
        d_in = fine(nt, out_map, d_score) + fine(tn, g_out, u_tail)
        grad[...] = leave * g_out + fine(nt, dy_lead, out_map)

        slope = sig * (1.0 + pre * (1.0 - sig))
        map_slope = map_sig * (1.0 + maps * (1.0 - map_sig))
        rest = g_ref.shape[0] - inner - STATE - slots
        rounded = jnp.concatenate(
            [
                (du * spread(step) + dy * gain_full) * slope,
                jnp.concatenate([d_in, d_out], axis=0) * map_slope,
                d_raw,
                jnp.zeros((rest, group), F32),
            ],
            axis=0,
        ).astype(BF16)
        maps_ref[0, :, at] = d_in * map_slope[:STATE]
        maps_ref[1, :, at] = d_out * map_slope[STATE:]
        g_ref[:inner, at] = rounded[:inner]
        g_ref[inner : inner + STATE, at] = jnp.zeros((STATE, group), BF16)
        g_ref[inner + STATE :, at] = rounded[top:]
        split_ref[lax.rem(k + core, 2), k // 2] = rounded
        acc[0] += d_raw
        acc[1] += d_log * (rate * step)
        acc[2] += gather_rows(dy * x)
        return carry

    gain_full = spread(jnp.broadcast_to(gain, (slots, group)))
    lax.fori_loop(0, chunks, backward, 0)
    lane = lax.broadcasted_iota(jnp.int32, head_ref.shape, 1)
    total = jnp.zeros(head_ref.shape, F32)
    for i in range(3):
        total = jnp.where(lane == i, jnp.sum(acc[i], axis=1, keepdims=True), total)
    head_ref[...] = total


def mixer(pre, dy, par, hp):
    chunks, inner, group = dy.shape
    slots = par.shape[1]
    return pl.pallas_call(
        functools.partial(mixer_kernel, hp),
        out_shape=(
            jax.ShapeDtypeStruct((pre.shape[0] - STATE, pre.shape[1]), BF16),
            jax.ShapeDtypeStruct((2, chunks // 2, pre.shape[0], group), BF16),
            jax.ShapeDtypeStruct((2, STATE, pre.shape[1]), F32),
            jax.ShapeDtypeStruct((slots, 128), F32),
        ),
        in_specs=[pl.BlockSpec(memory_space=pltpu.VMEM)] * 3,
        out_specs=(pl.BlockSpec(memory_space=pltpu.VMEM),) * 4,
        scratch_shapes=[
            pltpu.VMEM((chunks, inner, STATE), F32),
            pltpu.VMEM((inner, STATE), F32),
            pltpu.VMEM((3, slots, group), F32),
        ],
        compiler_params=pltpu.CompilerParams(vmem_limit_bytes=48 * 1024 * 1024),
        name="mixer",
    )(pre, dy, par)


def body(seqs, zeros, hidden, output_grad, input_weight, step_bias, decay_log, skip_gain):
    heads = step_bias.shape[0]
    hp = up(heads, seqs) // seqs
    slots = up(hp, 8)
    inner, full = hp * HEAD_DIM, heads * HEAD_DIM
    spare = seqs * hp - heads
    width = up(inner + STATE + slots, 128)
    me = lax.axis_index("seq")
    core = lax.rem(me, 2)
    mine = inner + STATE
    length, model = hidden.shape[1:]

    def own(array, axis, size, extra):
        if extra:
            pads = [(0, 0)] * array.ndim
            pads[axis] = (0, extra)
            array = jnp.pad(array, pads)
        return lax.dynamic_slice_in_dim(array, me * size, size, axis)

    weight = jnp.concatenate(
        [
            own(input_weight[:, :full], 1, inner, spare * HEAD_DIM),
            lax.dynamic_slice_in_dim(input_weight[:, full : full + 2 * STATE], core * STATE, STATE, 1),
            own(input_weight[:, full + 2 * STATE :], 1, hp, spare),
            jnp.zeros((input_weight.shape[0], width - mine - hp), BF16),
        ],
        axis=1,
    )
    cot = jnp.pad(output_grad[0], ((0, 0), (0, spare * HEAD_DIM))).T.reshape(seqs, inner, length)
    par = jnp.stack([own(v, 0, hp, spare) for v in (step_bias, decay_log, skip_gain)])
    par = jnp.broadcast_to(jnp.pad(par, ((0, 0), (0, slots - hp)))[:, :, None], (3, slots, 128))

    tokens, dy, columns, beside = collect(hidden[0], cot, weight, seqs, zeros)
    tokens = tokens.reshape(seqs * length, model)
    columns = columns.reshape(model, width)
    beside = beside.reshape(model, width)
    here, there = columns[:, inner:mine], beside[:, inner:mine]
    both = [jnp.where(core == 0, here, there), jnp.where(core == 0, there, here)]
    columns = jnp.concatenate([columns[:, :inner]] + both + [columns[:, mine:]], axis=1)
    beside = jnp.concatenate([beside[:, :inner]] + both + [beside[:, mine:]], axis=1)
    pre = lax.dot_general(columns, tokens, (((0,), (1,)), ((), ())), preferred_element_type=F32)
    grads, split, maps, sums = mixer(pre, dy, par, hp)
    other, other_map = swap(split, maps)
    pair_map = lax.dynamic_index_in_dim(maps, core, 0, False) + other_map
    grads = jnp.concatenate([grads[:inner], pair_map.astype(BF16), grads[mine:]], axis=0)

    def back(part, w):
        return lax.dot_general(part, w, (((1,), (1,)), ((), ())), preferred_element_type=F32)

    token_part = (back(split[0], columns) + back(other, beside)).astype(BF16)
    weight_part = lax.dot_general(
        tokens, grads, (((0,), (1,)), ((), ())), preferred_element_type=F32
    ).astype(BF16)
    every = seqs * zeros
    weight_part = weight_part.reshape(seqs, zeros, model // every, width)

    token_all, rows, sums_all = deliver(token_part, weight_part, sums, seqs, zeros)
    token_grad = jnp.sum(token_all.astype(F32), axis=0).astype(BF16)
    rows = rows.astype(F32)
    parts = rows.transpose(1, 0, 2)
    weight_grad = jnp.concatenate(
        [
            parts[:, :, :inner].reshape(-1, seqs * inner)[:, :full],
            jnp.sum(rows[0::2, :, inner:mine], axis=0),
            jnp.sum(rows[1::2, :, inner:mine], axis=0),
            parts[:, :, mine : mine + hp].reshape(-1, seqs * hp)[:, :heads],
        ],
        axis=1,
    )
    head_grads = sums_all[:, :hp, :3].transpose(2, 0, 1).reshape(3, seqs * hp)[:, :heads]
    return (token_grad[None], weight_grad, head_grads)


def solution(mesh):
    placed = (P("zero", "seq", None), P("zero", "seq", None), P("zero", None), P(), P(), P())
    return jax.shard_map(
        functools.partial(body, mesh.shape["seq"], mesh.shape["zero"]),
        mesh=mesh,
        in_specs=placed,
        out_specs=(P("zero", "seq", None), P(("seq", "zero"), None), P()),
        check_vma=False,
    )
```

```python
import functools

import jax
import jax.numpy as jnp
from jax import lax
from jax.experimental import pallas as pl
from jax.experimental.pallas import tpu as pltpu
from jax.sharding import PartitionSpec as P

HEAD_DIM = 64
STATE = 128
MESH = pl.DeviceIdType.MESH
F32 = jnp.float32
BF16 = jnp.bfloat16


def up(size, unit):
    return -(-size // unit) * unit


def nn(a, b):
    return lax.dot_general(a, b, (((1,), (0,)), ((), ())), preferred_element_type=F32)


def nt(a, b):
    return lax.dot_general(a, b, (((1,), (1,)), ((), ())), preferred_element_type=F32)


def tn(a, b):
    return lax.dot_general(a, b, (((0,), (0,)), ((), ())), preferred_element_type=F32)


def halves(a):
    high = a.astype(BF16)
    return high, (a - high.astype(F32)).astype(BF16)


def fine(dot, a, b):
    if a.dtype == BF16:
        high, low = halves(b)
        return dot(a, high) + dot(a, low)
    if b.dtype == BF16:
        high, low = halves(a)
        return dot(high, b) + dot(low, b)
    (ah, al), (bh, bl) = halves(a), halves(b)
    return dot(ah, bh) + (dot(al, bh) + dot(ah, bl))


def exact(a, b):
    return lax.dot_general(
        a, b, (((1,), (0,)), ((), ())), precision=lax.Precision.HIGHEST, preferred_element_type=F32
    )


def greet(peers):
    barrier = pltpu.get_barrier_semaphore()
    for peer in peers:
        pl.semaphore_signal(barrier, inc=1, device_id=peer, device_id_type=MESH)
    pl.semaphore_wait(barrier, len(peers))


def remote(src, dst, send, recv, peer):
    return pltpu.make_async_remote_copy(src, dst, send, recv, peer, MESH)


def collect_kernel(
    seqs, zeros, tok, cot, wgt, tok_out, cot_out, wgt_out, wsib_out,
    tsem, fsem, csem, rsem, ssem, loc,
):
    me_s, me_z = lax.axis_index("seq"), lax.axis_index("zero")
    chips = seqs // 2
    chip, core = me_s // 2, lax.rem(me_s, 2)
    sibling = (chip * 2 + 1 - core, me_z)
    half = wgt.shape[0] // 2
    full_hops = (zeros - 1) // 2
    upper, lower = pl.ds(0, half), pl.ds(half, wgt.shape[0] - half)

    def along(step):
        return (lax.rem(me_s + step, seqs), me_z)

    def owner(shift):
        return lax.rem(me_z + shift + zeros, zeros)

    right, left = (me_s, owner(1)), (me_s, owner(-1))
    greet([along(i) for i in range(1, seqs)] + ([right, left] if zeros > 1 else []))

    own = [
        pltpu.make_async_copy(tok, tok_out.at[me_s], loc.at[0]),
        pltpu.make_async_copy(cot.at[me_s], cot_out.at[me_s], loc.at[1]),
        pltpu.make_async_copy(wgt, wgt_out.at[me_z], loc.at[2]),
    ]

    def hop(way, h):
        at = owner(-way * (h - 1))
        src = wgt if h == 1 else wgt_out.at[at]
        dst = wgt_out.at[at]
        if h > full_hops:
            rows = upper if way > 0 else lower
            src, dst = src.at[rows], dst.at[rows]
        row = 0 if way > 0 else 2
        return remote(src, dst, rsem.at[row, h], rsem.at[row + 1, h], right if way > 0 else left)

    hops = full_hops + (1 - zeros % 2)
    ring = [(hop(1, h), hop(-1, h)) for h in range(1, hops + 1)]

    def token_slot(step):
        return lax.rem(chip - step + chips, chips) * 2 + core

    tokens = [
        remote(
            tok, tok_out.at[me_s], tsem.at[0, d], tsem.at[1, d],
            (lax.rem(chip + d, chips) * 2 + core, me_z),
        )
        for d in range(1, chips)
    ]
    cots = []
    for d in range(1, seqs):
        peer = along(d)
        cots.append(
            remote(cot.at[peer[0]], cot_out.at[me_s], csem.at[0, d], csem.at[1, d], peer)
        )
    passed = [remote(tok, tok_out.at[me_s], fsem.at[0, 0], fsem.at[1, 0], sibling)]
    for d in range(1, chips):
        at = token_slot(d)
        passed.append(remote(tok_out.at[at], tok_out.at[at], fsem.at[0, d], fsem.at[1, d], sibling))

    def share(slot, at, src):
        return remote(src, wsib_out.at[at], ssem.at[0, slot], ssem.at[1, slot], sibling)

    shared = [share(0, me_z, wgt)]
    for d in range(1, zeros):
        at = owner(-d)
        shared.append(share(d, at, wgt_out.at[at]))

    for copy in ring[0] if ring else ():
        copy.start()
    for copy in tokens + cots + [passed[0], shared[0]] + own:
        copy.start()
    for h in range(1, hops):
        for way in (0, 1):
            ring[h - 1][way].wait_recv()
            ring[h][way].start()
    for d in range(1, chips):
        tokens[d - 1].wait_recv()
        passed[d].start()
    if ring:
        for way in (0, 1):
            ring[-1][way].wait_recv()
    for copy in shared[1:]:
        copy.start()
    for pair in ring:
        for copy in pair:
            copy.wait_send()
    for copy in tokens:
        copy.wait_send()
    for copy in own + cots + passed + shared:
        copy.wait()


def collect(tok, cot, wgt, seqs, zeros):
    anywhere = pl.BlockSpec(memory_space=pl.ANY)
    columns = jax.ShapeDtypeStruct((zeros,) + wgt.shape, wgt.dtype)
    return pl.pallas_call(
        functools.partial(collect_kernel, seqs, zeros),
        out_shape=(
            jax.ShapeDtypeStruct((seqs,) + tok.shape, tok.dtype),
            jax.ShapeDtypeStruct(cot.shape, cot.dtype),
            columns,
            columns,
        ),
        in_specs=[anywhere] * 3,
        out_specs=(anywhere,) * 4,
        scratch_shapes=[
            pltpu.SemaphoreType.DMA((2, seqs)),
            pltpu.SemaphoreType.DMA((2, seqs)),
            pltpu.SemaphoreType.DMA((2, seqs)),
            pltpu.SemaphoreType.DMA((4, zeros + 1)),
            pltpu.SemaphoreType.DMA((2, zeros)),
            pltpu.SemaphoreType.DMA((3,)),
        ],
        compiler_params=pltpu.CompilerParams(collective_id=0, has_side_effects=True),
        name="collect",
    )(tok, cot, wgt)


def swap_kernel(give, maps, got, got_map, send, recv):
    me_s, me_z = lax.axis_index("seq"), lax.axis_index("zero")
    core = lax.rem(me_s, 2)
    sibling = (me_s // 2 * 2 + 1 - core, me_z)
    greet([sibling])
    copies = [
        remote(maps.at[1 - core], got_map, send.at[0], recv.at[0], sibling),
        remote(give.at[1], got, send.at[1], recv.at[1], sibling),
    ]
    for copy in copies:
        copy.start()
    for copy in copies:
        copy.wait()


def swap(split, maps):
    anywhere = pl.BlockSpec(memory_space=pl.ANY)
    return pl.pallas_call(
        swap_kernel,
        out_shape=(
            jax.ShapeDtypeStruct(split.shape[1:], split.dtype),
            jax.ShapeDtypeStruct(maps.shape[1:], maps.dtype),
        ),
        in_specs=[anywhere, anywhere],
        out_specs=(anywhere, anywhere),
        scratch_shapes=[pltpu.SemaphoreType.DMA((2,)), pltpu.SemaphoreType.DMA((2,))],
        compiler_params=pltpu.CompilerParams(collective_id=2, has_side_effects=True),
        name="swap",
    )(split, maps)


def deliver_kernel(
    seqs, zeros, tok, wgt, head, tok_out, wgt_out, head_out,
    zin, zsum, hin, hsum, tsem, zsem, wsem, hsem, gsem, loc,
):
    me_s, me_z = lax.axis_index("seq"), lax.axis_index("zero")
    chips = seqs // 2
    chip, core = me_s // 2, lax.rem(me_s, 2)
    greet(
        [(me_s, lax.rem(me_z + d, zeros)) for d in range(1, zeros)]
        + [(lax.rem(me_s + d, seqs), me_z) for d in range(1, seqs)]
    )
    across = []
    for d in range(1, zeros):
        target = lax.rem(me_z + d, zeros)
        across.append(
            remote(wgt.at[:, target], zin.at[d], zsem.at[0, d], zsem.at[1, d], (me_s, target))
        )
        across.append(remote(head, hin.at[d], hsem.at[0, d], hsem.at[1, d], (me_s, target)))
    tokens = []
    for d in range(1, chips):
        target = lax.rem(chip + d, chips)
        tokens.append(
            remote(
                tok.at[target], tok_out.at[chip], tsem.at[0, d], tsem.at[1, d],
                (target * 2 + core, me_z),
            )
        )
    own = [pltpu.make_async_copy(tok.at[chip], tok_out.at[chip], loc.at[0])]
    first = [
        pltpu.make_async_copy(wgt.at[:, me_z], zin.at[0], loc.at[2]),
        pltpu.make_async_copy(head, hin.at[0], loc.at[1]),
    ]
    for copy in across + tokens + first + own:
        copy.start()
    for copy in first + across:
        copy.wait()
    sums = hin[0]
    for d in range(1, zeros):
        sums = sums + hin[d]
    hsum[...] = sums

    def add(j, carry):
        total = zin[0, j].astype(F32)
        for d in range(1, zeros):
            total = total + zin[d, j].astype(F32)
        zsum[j] = total.astype(BF16)
        return carry

    lax.fori_loop(0, seqs, add, 0)
    own += [
        pltpu.make_async_copy(zsum.at[me_s], wgt_out.at[me_s], loc.at[3]),
        pltpu.make_async_copy(hsum, head_out.at[me_s], loc.at[4]),
    ]
    for copy in own[1:]:
        copy.start()
    along = []
    for d in range(1, seqs):
        target = lax.rem(me_s + d, seqs)
        along.append(
            remote(
                zsum.at[target], wgt_out.at[me_s], wsem.at[0, d], wsem.at[1, d], (target, me_z)
            )
        )
        along.append(
            remote(hsum, head_out.at[me_s], gsem.at[0, d], gsem.at[1, d], (target, me_z))
        )
    for copy in along:
        copy.start()
    for copy in own + tokens + along:
        copy.wait()


def deliver(tok, wgt, head, seqs, zeros):
    anywhere = pl.BlockSpec(memory_space=pl.ANY)
    block = wgt.shape[2:]
    return pl.pallas_call(
        functools.partial(deliver_kernel, seqs, zeros),
        out_shape=(
            jax.ShapeDtypeStruct(tok.shape, tok.dtype),
            jax.ShapeDtypeStruct((seqs,) + block, wgt.dtype),
            jax.ShapeDtypeStruct((seqs,) + head.shape, head.dtype),
        ),
        in_specs=[anywhere] * 3,
        out_specs=(anywhere,) * 3,
        scratch_shapes=[
            pltpu.VMEM((zeros, seqs) + block, BF16),
            pltpu.VMEM((seqs,) + block, BF16),
            pltpu.VMEM((zeros,) + head.shape, F32),
            pltpu.VMEM(head.shape, F32),
            pltpu.SemaphoreType.DMA((2, seqs)),
            pltpu.SemaphoreType.DMA((2, zeros)),
            pltpu.SemaphoreType.DMA((2, seqs)),
            pltpu.SemaphoreType.DMA((2, zeros)),
            pltpu.SemaphoreType.DMA((2, seqs)),
            pltpu.SemaphoreType.DMA((5,)),
        ],
        compiler_params=pltpu.CompilerParams(collective_id=1, has_side_effects=True),
        name="deliver",
    )(tok, wgt, head)


def mixer_kernel(hp, pre_ref, other_ref, dy_ref, par_ref, g_ref, split_ref, maps_ref, head_ref, states, grad, acc):
    chunks, inner, group = dy_ref.shape
    top = inner + STATE
    slots = acc.shape[1]
    core = lax.rem(lax.axis_index("seq"), 2)
    bias = par_ref[0][:, :1]
    rate = -jnp.exp(par_ref[1][:, :1])
    gain = par_ref[2][:, :1]
    row = lax.broadcasted_iota(jnp.int32, (group, group), 0)
    col = lax.broadcasted_iota(jnp.int32, (group, group), 1)
    causal = col >= row
    before = causal.astype(F32)
    after = (col <= row).astype(F32)

    def spread(rows):
        return jnp.concatenate(
            [jnp.broadcast_to(rows[h : h + 1], (HEAD_DIM, rows.shape[1])) for h in range(hp)], axis=0
        )

    def gather_rows(full):
        parts = [
            jnp.sum(full[h * HEAD_DIM : (h + 1) * HEAD_DIM], axis=0, keepdims=True) for h in range(hp)
        ]
        if slots > hp:
            parts.append(jnp.zeros((slots - hp, full.shape[1]), F32))
        return jnp.concatenate(parts, axis=0)

    def load(k):
        at = pl.ds(pl.multiple_of(k * group, group), group)
        pre = pre_ref[:inner, at]
        sig = jax.nn.sigmoid(pre)
        here, there = pre_ref[inner:top, at], other_ref[:, at]
        maps = jnp.concatenate(
            [jnp.where(core == 0, here, there), jnp.where(core == 0, there, here)], axis=0
        )
        map_sig = jax.nn.sigmoid(maps)
        raw = pre_ref[top : top + slots, at] + bias
        step = jax.nn.softplus(raw)
        cum = exact(rate * step, before)
        return at, pre, sig, maps, map_sig, raw, step, cum

    grad[...] = jnp.zeros_like(grad)

    def forward(k, carry):
        at, pre, sig, maps, map_sig, raw, step, cum = load(k)
        last = cum[:, group - 1 :]
        x = pre * sig
        in_map = maps[:STATE] * map_sig[:STATE]
        tail = x * spread(step * jnp.exp(last - cum))
        held = grad[...]
        states[k] = held
        grad[...] = spread(jnp.exp(jnp.broadcast_to(last, (slots, STATE)))) * held + fine(nt, tail, in_map)
        return carry

    lax.fori_loop(0, chunks, forward, 0)
    grad[...] = jnp.zeros_like(grad)
    acc[...] = jnp.zeros_like(acc)

    def backward(i, carry):
        k = chunks - 1 - i
        at, pre, sig, maps, map_sig, raw, step, cum = load(k)
        last = cum[:, group - 1 :]
        x = pre * sig
        both = maps * map_sig
        in_map = both[:STATE]
        out_map = both[STATE:]
        dy16 = dy_ref[k]
        dy = dy16.astype(F32)
        u = x * spread(step)
        tail = spread(jnp.exp(last - cum))
        lead = spread(jnp.exp(cum))
        leave = spread(jnp.exp(jnp.broadcast_to(last, (slots, STATE))))
        held = states[k]
        g_out = grad[...]
        u_tail = u * tail
        dy_lead = dy * lead

        score = fine(tn, in_map, out_map)
        cum_col = jnp.concatenate([cum, jnp.zeros((group - slots, group), F32)], axis=0).T
        d_score = jnp.zeros((group, group), F32)
        ksum = jnp.zeros((group, group), F32)
        du_parts = []
        r_parts = []
        for h in range(hp):
            at_h = slice(h * HEAD_DIM, (h + 1) * HEAD_DIM)
            diff = cum[h : h + 1] - cum_col[:, h : h + 1]
            within = jnp.where(causal, jnp.exp(jnp.where(causal, diff, 0.0)), 0.0)
            mixing = score * within
            d_mix = fine(tn, u[at_h], dy16[at_h])
            du_parts.append(fine(nt, dy16[at_h], mixing))
            d_score = d_score + d_mix * within
            pair = d_mix * mixing
            r_parts.append(jnp.sum(pair, axis=0, keepdims=True))
            ksum = jnp.where(col == h, jnp.sum(pair, axis=1, keepdims=True), ksum)
        if slots > hp:
            r_parts.append(jnp.zeros((slots - hp, group), F32))
        from_tail = fine(nn, g_out, in_map) * tail
        tail_rows = gather_rows(u * from_tail)
        lead_rows = gather_rows(dy_lead * fine(nn, held, out_map))
        du = jnp.concatenate(du_parts, axis=0) + from_tail
        d_cum = jnp.concatenate(r_parts, axis=0) - ksum.T[:slots] + lead_rows - tail_rows
        cross = jnp.sum(gather_rows(held * g_out * leave) + tail_rows, axis=1, keepdims=True)
        d_log = exact(d_cum, after) + cross
        d_step = gather_rows(du * x) + rate * d_log
        d_raw = d_step * jax.nn.sigmoid(raw)

        d_out = fine(nn, in_map, d_score) + fine(tn, held, dy_lead)
        d_in = fine(nt, out_map, d_score) + fine(tn, g_out, u_tail)
        grad[...] = leave * g_out + fine(nt, dy_lead, out_map)

        slope = sig * (1.0 + pre * (1.0 - sig))
        map_slope = map_sig * (1.0 + maps * (1.0 - map_sig))
        rest = g_ref.shape[0] - top - slots
        d_in = d_in * map_slope[:STATE]
        d_out = d_out * map_slope[STATE:]
        rounded = jnp.concatenate(
            [
                (du * spread(step) + dy * gain_full) * slope,
                jnp.where(core == 0, d_in, d_out),
                d_raw,
                jnp.zeros((rest, group), F32),
            ],
            axis=0,
        ).astype(BF16)
        g_ref[:, at] = rounded
        split_ref[lax.rem(k + core, 2), k // 2] = rounded
        maps_ref[0, :, at] = d_in
        maps_ref[1, :, at] = d_out
        acc[0] += d_raw
        acc[1] += d_log * (rate * step)
        acc[2] += gather_rows(dy * x)
        return carry

    gain_full = spread(jnp.broadcast_to(gain, (slots, group)))
    lax.fori_loop(0, chunks, backward, 0)
    lane = lax.broadcasted_iota(jnp.int32, head_ref.shape, 1)
    total = jnp.zeros(head_ref.shape, F32)
    for i in range(3):
        total = jnp.where(lane == i, jnp.sum(acc[i], axis=1, keepdims=True), total)
    head_ref[...] = total


def mixer(pre, other, dy, par, hp):
    chunks, inner, group = dy.shape
    slots = par.shape[1]
    return pl.pallas_call(
        functools.partial(mixer_kernel, hp),
        out_shape=(
            jax.ShapeDtypeStruct(pre.shape, BF16),
            jax.ShapeDtypeStruct((2, chunks // 2, pre.shape[0], group), BF16),
            jax.ShapeDtypeStruct((2, STATE, pre.shape[1]), F32),
            jax.ShapeDtypeStruct((slots, 128), F32),
        ),
        in_specs=[pl.BlockSpec(memory_space=pltpu.VMEM)] * 4,
        out_specs=(pl.BlockSpec(memory_space=pltpu.VMEM),) * 4,
        scratch_shapes=[
            pltpu.VMEM((chunks, inner, STATE), F32),
            pltpu.VMEM((inner, STATE), F32),
            pltpu.VMEM((3, slots, group), F32),
        ],
        compiler_params=pltpu.CompilerParams(vmem_limit_bytes=48 * 1024 * 1024),
        name="mixer",
    )(pre, other, dy, par)


def body(seqs, zeros, hidden, output_grad, input_weight, step_bias, decay_log, skip_gain):
    heads = step_bias.shape[0]
    hp = up(heads, seqs) // seqs
    slots = up(hp, 8)
    inner, full = hp * HEAD_DIM, heads * HEAD_DIM
    spare = seqs * hp - heads
    width = up(inner + STATE + slots, 128)
    me = lax.axis_index("seq")
    core = lax.rem(me, 2)
    mine = inner + STATE
    length, model = hidden.shape[1:]

    def own(array, axis, size, extra):
        if extra:
            pads = [(0, 0)] * array.ndim
            pads[axis] = (0, extra)
            array = jnp.pad(array, pads)
        return lax.dynamic_slice_in_dim(array, me * size, size, axis)

    weight = jnp.concatenate(
        [
            own(input_weight[:, :full], 1, inner, spare * HEAD_DIM),
            lax.dynamic_slice_in_dim(input_weight[:, full : full + 2 * STATE], core * STATE, STATE, 1),
            own(input_weight[:, full + 2 * STATE :], 1, hp, spare),
            jnp.zeros((input_weight.shape[0], width - mine - hp), BF16),
        ],
        axis=1,
    )
    cot = jnp.pad(output_grad[0], ((0, 0), (0, spare * HEAD_DIM))).T.reshape(seqs, inner, length)
    par = jnp.stack([own(v, 0, hp, spare) for v in (step_bias, decay_log, skip_gain)])
    par = jnp.broadcast_to(jnp.pad(par, ((0, 0), (0, slots - hp)))[:, :, None], (3, slots, 128))

    tokens, dy, columns, beside = collect(hidden[0], cot, weight, seqs, zeros)
    tokens = tokens.reshape(seqs * length, model)
    columns = columns.reshape(model, width)
    beside = beside.reshape(model, width)
    pre = lax.dot_general(columns, tokens, (((0,), (1,)), ((), ())), preferred_element_type=F32)
    other_pre = lax.dot_general(
        beside[:, inner:mine], tokens, (((0,), (1,)), ((), ())), preferred_element_type=F32
    )
    grads, split, maps, sums = mixer(pre, other_pre, dy, par, hp)
    other, other_map = swap(split, maps)
    pair_map = lax.dynamic_index_in_dim(maps, core, 0, False) + other_map
    grads = jnp.concatenate([grads[:inner], pair_map.astype(BF16), grads[mine:]], axis=0)

    def back(part, w):
        return lax.dot_general(part, w, (((1,), (1,)), ((), ())), preferred_element_type=F32)

    def parity(m):
        m = m.reshape(STATE, seqs // 2, 2, length)
        return lax.dynamic_index_in_dim(m, core, 2, False).transpose(1, 0, 2)

    def filled(part, middle):
        return jnp.concatenate([part[:, :inner], middle.astype(BF16), part[:, mine:]], axis=1)

    first = filled(split[0], parity(pair_map))
    rest_map = lax.dynamic_index_in_dim(maps, 1 - core, 0, False)
    second = filled(other, other[:, inner:mine].astype(F32) + parity(rest_map))
    token_part = (back(first, columns) + back(second, beside)).astype(BF16)
    weight_part = lax.dot_general(
        tokens, grads, (((0,), (1,)), ((), ())), preferred_element_type=F32
    ).astype(BF16)
    every = seqs * zeros
    weight_part = weight_part.reshape(seqs, zeros, model // every, width)

    token_all, rows, sums_all = deliver(token_part, weight_part, sums, seqs, zeros)
    token_grad = jnp.sum(token_all.astype(F32), axis=0).astype(BF16)
    rows = rows.astype(F32)
    parts = rows.transpose(1, 0, 2)
    weight_grad = jnp.concatenate(
        [
            parts[:, :, :inner].reshape(-1, seqs * inner)[:, :full],
            jnp.sum(rows[0::2, :, inner:mine], axis=0),
            jnp.sum(rows[1::2, :, inner:mine], axis=0),
            parts[:, :, mine : mine + hp].reshape(-1, seqs * hp)[:, :heads],
        ],
        axis=1,
    )
    head_grads = sums_all[:, :hp, :3].transpose(2, 0, 1).reshape(3, seqs * hp)[:, :heads]
    return (token_grad[None], weight_grad, head_grads)


def solution(mesh):
    placed = (P("zero", "seq", None), P("zero", "seq", None), P("zero", None), P(), P(), P())
    return jax.shard_map(
        functools.partial(body, mesh.shape["seq"], mesh.shape["zero"]),
        mesh=mesh,
        in_specs=placed,
        out_specs=(P("zero", "seq", None), P(("seq", "zero"), None), P()),
        check_vma=False,
    )
```
